128 devices in a mesh: mx: 4 (over z), my: 4 (over y_hi, core), col: 8 (over y_lo, x).
Axes of the slice: x: 4, y: 4 (y_hi: 2, y_lo: 2; y = y_hi * 2 + y_lo), z: 4, core: 2. Of those that a mesh axis runs over, the one named last changes fastest.
Arguments:
- spectrum: float32 [2, 16, 128, 32, 512], P(None, 'col', None, 'mx', 'my'), may hold values from -6 to 6
- core_tensor: float32 [2, 64, 64, 16, 16, 16], P(None, 'col', None, ('mx', 'my')), may hold values from -0.01171875 to 0.01171875
- input_factor: float32 [128, 64], replicated, may hold values from -0.5 to 0.5
- output_factor: float32 [128, 64], replicated, may hold values from -0.75 to 0.75
- first_factor: float32 [32, 16], P('mx'), may hold values from -5 to 5
- second_factor: float32 [32, 16], P('my'), may hold values from -5 to 5
- third_factor: float32 [16, 16], replicated, may hold values from -5 to 5
Outputs:
- mixed_modes: float32 [2, 16, 128, 32, 512], P(None, 'col', None, 'mx', 'my')
The draws below stay inside these ranges and needn't reach their ends.
All inputs are finite; a program needn't handle non-finite values.
Results may differ from the reference program's by a relative error of at most 0.00007.
Values sent between devices are 32-bit elements; how exact they have to be, the bound alone decides.
A program may use at most 128 MiB of HBM per device.

```python
import jax
import jax.numpy as jnp
from jax import lax

CIN = 128
COUT = 128
R1 = 64
R2 = 64
R3 = 16
R4 = 16
R5 = 16
KX = 32
KY = 32
KZ = 16
BATCH = 16


def block_scale(key, extent, split, low, largest):
    level, own = 1.0, jax.random.fold_in(key, 6)
    for dim, blocks in split:
        steps = jnp.exp(jax.random.uniform(jax.random.fold_in(own, dim), (blocks,), jnp.float32, low / len(split), largest / len(split)))
        level = level * jnp.repeat(steps, extent[dim] // blocks).reshape([-1 if axis == dim else 1 for axis in range(len(extent))])
    return level


def bell_draw(own_key, shape, width, most, split=(), held_as=jnp.bfloat16):
    values = width * jax.random.normal(own_key, shape, jnp.float32)
    if split:
        values = values * block_scale(own_key, shape, split, -0.22, 0.18)
    return jnp.clip(values, -most, most).astype(held_as)


def setup_inputs(seed: int = 0) -> dict:
    arg_keys = jax.random.split(jax.random.key(seed), 8)
    spectrum = bell_draw(arg_keys[0], (2, BATCH, CIN, KX, KY * KZ), 1.0, 6.0, ((1, 8), (3, 4), (4, 4)), jnp.float32)
    core_tensor = bell_draw(arg_keys[1], (2, R1, R2, R3, R4, R5), (R1 * R3 * R4 * R5) ** -0.5, 0.01171875, ((1, 8), (3, 16)), jnp.float32)
    input_factor = bell_draw(arg_keys[2], (CIN, R1), CIN ** -0.5, 0.5, (), jnp.float32)
    output_factor = bell_draw(arg_keys[3], (COUT, R2), R2 ** -0.5, 0.75, (), jnp.float32)
    first_factor = bell_draw(arg_keys[4], (KX, R3), 1.0, 5.0, ((0, 4),), jnp.float32)
    second_factor = bell_draw(arg_keys[5], (KY, R4), 1.0, 5.0, ((0, 4),), jnp.float32)
    third_factor = bell_draw(arg_keys[6], (KZ, R5), 1.0, 5.0, (), jnp.float32)
    return {"spectrum": spectrum, "core_tensor": core_tensor, "input_factor": input_factor, "output_factor": output_factor, "first_factor": first_factor, "second_factor": second_factor, "third_factor": third_factor}


def reference(spectrum, core_tensor, input_factor, output_factor, first_factor, second_factor, third_factor):
    precise = lax.Precision.HIGHEST
    rank_spectrum = jnp.einsum('cbikm,ir->cbrkm', spectrum, input_factor, precision=precise)
    core_third = jnp.einsum('cpqstu,zu->cpqstz', core_tensor, third_factor, precision=precise)
    core_second = jnp.einsum('cpqstz,yt->cpqsyz', core_third, second_factor, precision=precise)
    core_second = core_second.reshape(2, R1, R2, R3, KY * KZ)

    def per_mode_row(inputs):
        spectrum_row, factor_row = inputs
        weight_row = jnp.einsum('cpqsm,s->cpqm', core_second, factor_row, precision=precise)
        real_part = jnp.einsum('brm,rqm->bqm', spectrum_row[0], weight_row[0], precision=precise) - jnp.einsum('brm,rqm->bqm', spectrum_row[1], weight_row[1], precision=precise)
        imag_part = jnp.einsum('brm,rqm->bqm', spectrum_row[0], weight_row[1], precision=precise) + jnp.einsum('brm,rqm->bqm', spectrum_row[1], weight_row[0], precision=precise)
        mode_values = jnp.stack([real_part, imag_part])
        return jnp.einsum('oq,cbqm->cbom', output_factor, mode_values, precision=precise)

    mixed_rows = lax.map(per_mode_row, (jnp.moveaxis(rank_spectrum, 3, 0), first_factor))
    return jnp.moveaxis(mixed_rows, 0, 3)
```

```python
import jax
import jax.numpy as jnp
from jax import lax
from jax.sharding import PartitionSpec as P

precise = lax.Precision.HIGHEST


def per_device(
    spectrum, core_tensor, input_factor, output_factor, first_factor, second_factor, third_factor
):
    first = lax.all_gather(first_factor, "mx", axis=0, tiled=True)
    second = lax.all_gather(second_factor, "my", axis=0, tiled=True)
    pair = (second[:, None, :, None] * third_factor[None, :, None, :]).reshape(512, 256)
    core = core_tensor.reshape(2, 8, 64, 256)
    part = jnp.einsum("mk,cpqk->mpcq", pair, core, precision=precise).reshape(128, 4, 8, 128)
    part = lax.all_to_all(part, ("my", "mx", "col"), split_axis=0, concat_axis=0, tiled=True)
    part = part.reshape(4, 4, 8, 4, 8, 2, 64)
    ranked = jnp.einsum("cbikm,ip->mbkcp", spectrum, input_factor, precision=precise)
    ranked = ranked.reshape(32, 4, 16, 128)
    ranked = lax.all_to_all(ranked, ("mx", "col"), split_axis=0, concat_axis=0, tiled=True)
    ranked = ranked.reshape(4, 8, 4, 2, 8, 2, 64)
    firsts = first.reshape(4, 8, 4, 4)
    weight = jnp.einsum("xkst,tsdjpcq->jxkdpcq", firsts, part, precision=precise)
    weight = weight.reshape(4, 4, 8, 64, 2, 64)
    turned = jnp.stack([-weight[..., 1, :], weight[..., 0, :]], axis=-2)
    full = jnp.stack([weight, turned], axis=3).reshape(4, 4, 8, 128, 128)
    ranked = ranked.reshape(4, 8, 4, 2, 8, 128)
    values = jnp.einsum("xdjbkr,jxkrn->xdjbkn", ranked, full, precision=precise)
    values = values.reshape(32, 4, 16, 128)
    values = lax.all_to_all(values, ("mx", "col"), split_axis=0, concat_axis=0, tiled=True)
    values = values.reshape(128, 2, 8, 2, 64)
    return jnp.einsum("oq,mbkcq->cbokm", output_factor, values, precision=precise)


def solution(mesh):
    placed = (
        P(None, "col", None, "mx", "my"),
        P(None, "col", None, ("mx", "my"), None, None),
        P(),
        P(),
        P("mx", None),
        P("my", None),
        P(),
    )
    return jax.shard_map(
        per_device,
        mesh=mesh,
        in_specs=placed,
        out_specs=P(None, "col", None, "mx", "my"),
        check_vma=False,
    )
```

```python
import jax
import jax.numpy as jnp
from jax import lax
from jax.experimental import pallas as pl
from jax.experimental.pallas import tpu as pltpu
from jax.sharding import PartitionSpec as P

MESH = pl.DeviceIdType.MESH
HIGH = lax.Precision.HIGH
HIGHEST = lax.Precision.HIGHEST
F32 = jnp.float32


def dot(a, b, dims=((1,), (0,)), precision=HIGH):
    return lax.dot_general(a, b, (dims, ((), ())), precision=precision, preferred_element_type=F32)


def iota(shape, dim):
    return lax.broadcasted_iota(jnp.int32, shape, dim)


def kernel(
    spec_hbm, core_hbm, fin_ref, fout_ref, first_ref, second_ref, third_ref,
    out_ref,
    spec, core, xs, xr, bs, br, cs, cr, ys, yr, stage, fr, sr, m1, m2, gout, coef,
    in_sem, fac_send, fac_recv, b_send, b_recv, x_send, x_recv, c_send, c_recv, y_send, y_recv,
):
    z, my, col = lax.axis_index("mx"), lax.axis_index("my"), lax.axis_index("col")
    h, e = my // 2, my % 2
    l, x = col // 4, col % 4
    kz = z * 4 + x

    load_spec = pltpu.make_async_copy(spec_hbm, spec, in_sem.at[0])
    load_core = pltpu.make_async_copy(core_hbm, core, in_sem.at[1])
    load_core.start()
    load_spec.start()

    def plane(i):
        d = i + 1
        return (z + d // 8) % 4, my, ((l + (d // 4) % 2) % 2) * 4 + (x + d % 4) % 4

    def square(i):
        d = i + 1
        return z, ((h + d // 4) % 2) * 2 + (e + d % 2) % 2, ((l + (d // 2) % 2) % 2) * 4 + x

    barrier = pltpu.get_barrier_semaphore()

    def greet_plane(i, carry):
        pl.semaphore_signal(barrier, inc=1, device_id=plane(i), device_id_type=MESH)
        return carry

    def greet_square(i, carry):
        d = i + jnp.where(i >= 1, 1, 0)
        pl.semaphore_signal(barrier, inc=1, device_id=square(d), device_id_type=MESH)
        return carry

    lax.fori_loop(0, 31, greet_plane, 0)
    lax.fori_loop(0, 6, greet_square, 0)

    stage[...] = jnp.zeros_like(stage)
    stage[0, :, 0:16] = first_ref[...]
    stage[1, :, 0:16] = second_ref[...]
    fr[pl.ds(z, 1)] = stage[0:1]
    sr[pl.ds(my, 1)] = stage[1:2]

    spread = jnp.where(iota((16, 256), 1) % 16 == iota((16, 256), 0), 1.0, 0.0)
    wide = dot(third_ref[...], spread, precision=HIGHEST)
    wide = jnp.broadcast_to(wide[:, None, :], (16, 16, 256)).reshape(256, 256)
    m1[...] = jnp.where(iota((256, 256), 0) % 16 == iota((256, 256), 1) // 16, wide, 0.0)

    load_core.wait()

    def third_step(p, carry):
        both = jnp.concatenate([core[0, p], core[1, p]], axis=1)
        bs[:, p] = dot(m1[...], both).reshape(16, 16, 128)
        return carry

    lax.fori_loop(0, 8, third_step, 0)
    pl.semaphore_wait(barrier, 37)

    def send_first(i, carry):
        pltpu.make_async_remote_copy(
            stage.at[0], fr.at[z], fac_send.at[0], fac_recv.at[0],
            device_id=((z + i + 1) % 4, my, col), device_id_type=MESH,
        ).start()
        d = i + 1
        pltpu.make_async_remote_copy(
            stage.at[1], sr.at[my], fac_send.at[1], fac_recv.at[1],
            device_id=(z, ((h + d // 2) % 2) * 2 + (e + d % 2) % 2, col), device_id_type=MESH,
        ).start()
        return carry

    lax.fori_loop(0, 3, send_first, 0)

    def send_b(i, carry):
        d = i + 1
        tz, tx = (z + d // 4) % 4, (x + d % 4) % 4
        pltpu.make_async_remote_copy(
            bs.at[tz * 4 + tx], br.at[z, x], b_send, b_recv,
            device_id=(tz, my, l * 4 + tx), device_id_type=MESH,
        ).start()
        return carry

    lax.fori_loop(0, 15, send_b, 0)
    br[z, x] = bs[kz]

    load_spec.wait()
    xs2 = xs.reshape(2048, 128)

    def project(bk, carry):
        b, k = bk // 8, bk % 8
        real = dot(fin_ref[...], spec[pl.ds(b * 1024 + k, 128, stride=8), :])
        imag = dot(fin_ref[...], spec[pl.ds((2 + b) * 1024 + k, 128, stride=8), :])
        xs2[pl.ds(bk, 128, stride=16), :] = jnp.concatenate([real, imag], axis=0).T
        return carry

    lax.fori_loop(0, 16, project, 0)

    def send_x(i, carry):
        tz, tmy, tcol = plane(i)
        pltpu.make_async_remote_copy(
            xs.at[tcol // 4, :, tz * 4 + tcol % 4], xr.at[:, z * 8 + col], x_send, x_recv,
            device_id=(tz, tmy, tcol), device_id_type=MESH,
        ).start()
        return carry

    lax.fori_loop(0, 31, send_x, 0)
    for j in range(4):
        xr[j, z * 8 + col] = xs[l, j, kz]

    pltpu.make_async_copy(sr.at[0:3], sr.at[0:3], fac_recv.at[1]).wait()
    spread2 = jnp.where(iota((128, 128), 1) % 16 == iota((128, 128), 0), 1.0, 0.0)
    wide2 = dot(sr[...].reshape(32, 128), spread2, precision=HIGHEST)
    wide2 = jnp.broadcast_to(wide2[:, None, :], (32, 8, 128)).reshape(256, 128)
    m2[...] = jnp.where(iota((256, 128), 0) % 8 == iota((256, 128), 1) // 16, wide2, 0.0)

    pltpu.make_async_copy(bs.at[0:15], bs.at[0:15], b_recv).wait()

    def second_step(i, carry):
        zs, xsrc = i // 4, i % 4
        block = br[zs, xsrc].reshape(128, 128)
        cs[:, :, zs, pl.ds(xsrc * 8, 8), :] = dot(m2[...], block).reshape(8, 4, 8, 128)
        return carry

    lax.fori_loop(0, 16, second_step, 0)

    def send_c(n, carry):
        j, i = n // 7, n % 7
        tz, tmy, tcol = square(i)
        pltpu.make_async_remote_copy(
            cs.at[tmy * 2 + tcol // 4, j], cr.at[j, :, my, pl.ds(l * 32, 32), :],
            c_send, c_recv.at[j],
            device_id=(tz, tmy, tcol), device_id_type=MESH,
        ).start()
        return carry

    lax.fori_loop(0, 28, send_c, 0)

    def keep_c(n, carry):
        j, zs = n // 4, n % 4
        cr[j, zs, my, pl.ds(l * 32, 32), :] = cs[my * 2 + l, j, zs]
        return carry

    lax.fori_loop(0, 16, keep_c, 0)

    gout[...] = jnp.zeros_like(gout)
    turned = fout_ref[...].T
    gout[0:128, 0:64] = turned
    gout[128:256, 64:128] = turned
    pltpu.make_async_copy(sr.at[0:3], sr.at[0:3], fac_recv.at[0]).wait()
    for s in range(16):
        coef[s] = jnp.broadcast_to(fr[...].reshape(32, 128)[:, s : s + 1], (32, 128))
    pltpu.make_async_copy(xr.at[:, 0:31], xr.at[:, 0:31], x_recv).wait()

    sign = jnp.where(iota((64, 128), 1) < 64, -1.0, 1.0)

    def mode_step(j, carry):
        pltpu.make_async_copy(cs.at[0:7, 0], cs.at[0:7, 0], c_recv.at[j]).wait()
        rows = xr[j].reshape(512, 128)

        def group(g, inner):
            parts = []
            for i in range(4):
                top = cr[j, g, i]
                parts.append(jnp.concatenate([top, pltpu.roll(top, 64, 1) * sign], axis=0))
            prod = dot(rows, jnp.concatenate(parts, axis=1))
            total = None
            for i in range(4):
                piece = prod[:, i * 128 : (i + 1) * 128].reshape(4, 16, 8, 128)
                term = piece * coef[g * 4 + i].reshape(4, 1, 8, 128)
                total = term if total is None else total + term
            total = total.reshape(32, 16, 128)

            @pl.when(g == 0)
            def _():
                ys[j] = total

            @pl.when(g > 0)
            def _():
                ys[j] += total

            return inner

        lax.fori_loop(0, 4, group, 0)

        def send_y(i, inner):
            tz, tmy, tcol = plane(i)
            pltpu.make_async_remote_copy(
                ys.at[j, tz * 8 + tcol], yr.at[l, j, kz], y_send, y_recv,
                device_id=(tz, tmy, tcol), device_id_type=MESH,
            ).start()
            return inner

        lax.fori_loop(0, 31, send_y, 0)
        yr[l, j, kz] = ys[j, z * 8 + col]
        return carry

    lax.fori_loop(0, 4, mode_step, 0)
    pltpu.make_async_copy(ys.at[:, 0:31], ys.at[:, 0:31], y_recv).wait()
    yr2 = yr.reshape(2048, 128)

    def finish(bk, carry):
        b, k = bk // 8, bk % 8
        modes = yr2[pl.ds(bk, 128, stride=16), :]
        mixed = dot(gout[...], modes, ((1,), (1,)))
        out_ref[pl.ds(b * 1024 + k, 128, stride=8), :] = mixed[0:128]
        out_ref[pl.ds((2 + b) * 1024 + k, 128, stride=8), :] = mixed[128:256]
        return carry

    lax.fori_loop(0, 16, finish, 0)

    pltpu.make_async_copy(sr.at[0:3], sr.at[0:3], fac_send.at[0]).wait()
    pltpu.make_async_copy(sr.at[0:3], sr.at[0:3], fac_send.at[1]).wait()
    pltpu.make_async_copy(bs.at[0:15], bs.at[0:15], b_send).wait()
    pltpu.make_async_copy(xr.at[:, 0:31], xr.at[:, 0:31], x_send).wait()
    pltpu.make_async_copy(cs.at[0:7], cs.at[0:7], c_send).wait()
    pltpu.make_async_copy(ys.at[:, 0:31], ys.at[:, 0:31], y_send).wait()


def per_device(
    spectrum, core_tensor, input_factor, output_factor, first_factor, second_factor, third_factor
):
    spec = spectrum.reshape(4096, 128)
    core = jnp.transpose(core_tensor[:, :, :, 0], (0, 1, 3, 4, 2)).reshape(2, 8, 256, 64)
    anywhere = pl.BlockSpec(memory_space=pl.ANY)
    near = pl.BlockSpec(memory_space=pltpu.VMEM)
    vmem = lambda *shape: pltpu.VMEM(shape, F32)
    dma = pltpu.SemaphoreType.DMA
    out = pl.pallas_call(
        kernel,
        out_shape=jax.ShapeDtypeStruct((4096, 128), F32),
        in_specs=[anywhere, anywhere] + [near] * 5,
        out_specs=near,
        scratch_shapes=[
            vmem(4096, 128),
            vmem(2, 8, 256, 64),
            vmem(2, 4, 16, 16, 128),
            vmem(4, 32, 16, 128),
            vmem(16, 8, 16, 128),
            vmem(4, 4, 8, 16, 128),
            vmem(8, 4, 4, 32, 128),
            vmem(4, 4, 4, 64, 128),
            vmem(4, 32, 16, 128),
            vmem(2, 4, 16, 16, 128),
            vmem(2, 8, 128),
            vmem(4, 8, 128),
            vmem(4, 8, 128),
            vmem(256, 256),
            vmem(256, 128),
            vmem(256, 128),
            vmem(16, 32, 128),
            dma((2,)), dma((2,)), dma((2,)), dma, dma, dma, dma, dma, dma((4,)), dma, dma,
        ],
        compiler_params=pltpu.CompilerParams(
            collective_id=0, has_side_effects=True, vmem_limit_bytes=60 * 1024 * 1024
        ),
    )(spec, core, input_factor.T, output_factor.T, first_factor, second_factor, third_factor)
    return out.reshape(2, 2, 128, 8, 128)


def solution(mesh):
    placed = (
        P(None, "col", None, "mx", "my"),
        P(None, "col", None, ("mx", "my"), None, None),
        P(),
        P(),
        P("mx", None),
        P("my", None),
        P(),
    )
    return jax.shard_map(
        per_device,
        mesh=mesh,
        in_specs=placed,
        out_specs=P(None, "col", None, "mx", "my"),
        check_vma=False,
    )
```

```python
import jax
import jax.numpy as jnp
from jax import lax
from jax.experimental import pallas as pl
from jax.experimental.pallas import tpu as pltpu
from jax.sharding import PartitionSpec as P

MESH = pl.DeviceIdType.MESH
HIGH = lax.Precision.HIGH
HIGHEST = lax.Precision.HIGHEST
F32 = jnp.float32


def dot(a, b, dims=((1,), (0,)), precision=HIGH):
    return lax.dot_general(a, b, (dims, ((), ())), precision=precision, preferred_element_type=F32)


def iota(shape, dim):
    return lax.broadcasted_iota(jnp.int32, shape, dim)


def kernel(
    spec_hbm, core_hbm, fin_hbm, first_hbm, second_hbm, third_hbm,
    yr,
    spec, core, fin_ref, fin, first_ref, second_ref, third_ref, xs, xp, xr, bs, br, cs, cr, ys, stage, fr, sr, m1, m2, coef,
    in_sem, fac_send, fac_recv, b_send, b_recv, p_send, p_recv, x_send, x_recv, c_send, c_recv, y_send, y_recv, y_own,
):
    z, my, col = lax.axis_index("mx"), lax.axis_index("my"), lax.axis_index("col")
    h, e = my // 2, my % 2
    l, x = col // 4, col % 4
    kz = z * 4 + x

    loads = [
        pltpu.make_async_copy(far, here, in_sem.at[n])
        for n, (far, here) in enumerate((
            (fin_hbm, fin_ref), (spec_hbm, spec), (first_hbm, first_ref),
            (second_hbm, second_ref), (third_hbm, third_ref), (core_hbm, core),
        ))
    ]
    for load in loads:
        load.start()

    def plane(i):
        d = i + 1
        return (z + d // 8) % 4, my, ((l + (d // 4) % 2) % 2) * 4 + (x + d % 4) % 4

    def square(i):
        d = i + 1
        return z, ((h + d // 4) % 2) * 2 + (e + d % 2) % 2, ((l + (d // 2) % 2) % 2) * 4 + x

    barrier = pltpu.get_barrier_semaphore()

    def greet_plane(i, carry):
        pl.semaphore_signal(barrier, inc=1, device_id=plane(i), device_id_type=MESH)
        return carry

    def greet_square(i, carry):
        d = i + jnp.where(i >= 1, 1, 0)
        pl.semaphore_signal(barrier, inc=1, device_id=square(d), device_id_type=MESH)
        return carry

    lax.fori_loop(0, 31, greet_plane, 0)
    lax.fori_loop(0, 6, greet_square, 0)

    loads[0].wait()
    loads[1].wait()
    for a in range(16):
        true = (a // 8) * 32 + (a % 4) * 8 + (a // 4 % 2) * 4
        fin[4 * a : 4 * a + 4, :] = fin_ref[true : true + 4, :]
    xs2 = xs.reshape(2048, 128)

    def project(bk, carry):
        b, k = bk // 8, bk % 8
        real = dot(fin[...], spec[pl.ds(b * 1024 + k, 128, stride=8), :])
        imag = dot(fin[...], spec[pl.ds((2 + b) * 1024 + k, 128, stride=8), :])
        xs2[pl.ds(bk, 128, stride=16), :] = jnp.concatenate([real, imag], axis=0).T
        return carry

    lax.fori_loop(0, 16, project, 0)

    for load in loads[2:5]:
        load.wait()
    stage[...] = jnp.zeros_like(stage)
    stage[0, :, 0:16] = first_ref[...]
    stage[1, :, 0:16] = second_ref[...]
    fr[pl.ds(z, 1)] = stage[0:1]
    sr[pl.ds(my, 1)] = stage[1:2]

    pl.semaphore_wait(barrier, 37)

    swap = pltpu.make_async_remote_copy(
        xs.at[1 - l], xp, p_send, p_recv,
        device_id=(z, my, (1 - l) * 4 + x), device_id_type=MESH,
    )
    swap.start()

    def send_first(i, carry):
        pltpu.make_async_remote_copy(
            stage.at[0], fr.at[z], fac_send.at[0], fac_recv.at[0],
            device_id=((z + i + 1) % 4, my, col), device_id_type=MESH,
        ).start()
        d = i + 1
        pltpu.make_async_remote_copy(
            stage.at[1], sr.at[my], fac_send.at[1], fac_recv.at[1],
            device_id=(z, ((h + d // 2) % 2) * 2 + (e + d % 2) % 2, col), device_id_type=MESH,
        ).start()
        return carry

    lax.fori_loop(0, 3, send_first, 0)

    spread = jnp.where(iota((16, 256), 1) % 16 == iota((16, 256), 0), 1.0, 0.0)
    wide = dot(third_ref[...], spread, precision=HIGHEST)
    wide = jnp.broadcast_to(wide[:, None, :], (16, 16, 256)).reshape(256, 256)
    m1[...] = jnp.where(iota((256, 256), 0) % 16 == iota((256, 256), 1) // 16, wide, 0.0)
    loads[5].wait()

    def first_exchange(half, carry):
        def third_step(p, inner):
            both = jnp.concatenate([core[0, half * 4 + p], core[1, half * 4 + p]], axis=1)
            bs[:, half, p] = dot(m1[...], both).reshape(16, 16, 128)
            return inner

        lax.fori_loop(0, 4, third_step, 0)

        def send_b(i, inner):
            d = i + 1
            tz, tx = (z + d // 4) % 4, (x + d % 4) % 4
            pltpu.make_async_remote_copy(
                bs.at[tz * 4 + tx, half], br.at[half, z, x], b_send, b_recv.at[half],
                device_id=(tz, my, l * 4 + tx), device_id_type=MESH,
            ).start()
            return inner

        lax.fori_loop(0, 15, send_b, 0)
        br[half, z, x] = bs[kz, half]
        return carry

    lax.fori_loop(0, 2, first_exchange, 0)

    pltpu.make_async_copy(sr.at[0:3], sr.at[0:3], fac_recv.at[1]).wait()
    spread2 = jnp.where(iota((128, 128), 1) % 16 == iota((128, 128), 0), 1.0, 0.0)
    wide2 = dot(sr[...].reshape(32, 128), spread2, precision=HIGHEST)
    wide2 = jnp.broadcast_to(wide2[:, None, :], (32, 8, 128)).reshape(256, 128)
    m2[...] = jnp.where(iota((256, 128), 0) % 8 == iota((256, 128), 1) // 16, wide2, 0.0)

    def send_x(source, sample):
        def step(i, carry):
            d = i + 1
            tz, tx = (z + d // 4) % 4, (x + d % 4) % 4
            pltpu.make_async_remote_copy(
                source.at[:, tz * 4 + tx], xr.at[:, sample], x_send, x_recv,
                device_id=(tz, my, l * 4 + tx), device_id_type=MESH,
            ).start()
            return carry

        lax.fori_loop(0, 15, step, 0)
        for j in range(4):
            xr[j, sample] = source[j, kz]

    for half in range(2):
        pltpu.make_async_copy(bs.at[0:15, 0], bs.at[0:15, 0], b_recv.at[half]).wait()
        if half == 1:
            send_x(xs.at[l], z * 8 + col)

        def second_step(i, carry, half=half):
            zs, pair = i // 2, i % 2
            block = br[half, zs, pl.ds(pair * 2, 2)].reshape(128, 128)
            cs[half, :, :, zs, pl.ds(pair * 8, 8), :] = dot(m2[...], block).reshape(8, 4, 8, 128)
            return carry

        lax.fori_loop(0, 8, second_step, 0)

        def send_c(n, carry, half=half):
            j, i = n // 7, n % 7
            tz, tmy, tcol = square(i)
            pltpu.make_async_remote_copy(
                cs.at[half, tmy * 2 + tcol // 4, j],
                cr.at[j, :, my, pl.ds(l * 32 + half * 16, 16), :],
                c_send, c_recv.at[j],
                device_id=(tz, tmy, tcol), device_id_type=MESH,
            ).start()
            return carry

        lax.fori_loop(0, 28, send_c, 0)

        def keep_c(n, carry, half=half):
            j, zs = n // 4, n % 4
            cr[j, zs, my, pl.ds(l * 32 + half * 16, 16), :] = cs[half, my * 2 + l, j, zs]
            return carry

        lax.fori_loop(0, 16, keep_c, 0)

    swap.wait()
    send_x(xp, z * 8 + (1 - l) * 4 + x)

    pltpu.make_async_copy(sr.at[0:3], sr.at[0:3], fac_recv.at[0]).wait()
    for s in range(16):
        coef[s] = jnp.broadcast_to(fr[...].reshape(32, 128)[:, s : s + 1], (32, 128))
    pltpu.make_async_copy(xr.at[:, 0:30], xr.at[:, 0:30], x_recv).wait()

    sign = jnp.where(iota((64, 128), 1) < 64, -1.0, 1.0)

    def mode_step(j, carry):
        pltpu.make_async_copy(cs.at[:, 0:7, 0], cs.at[:, 0:7, 0], c_recv.at[j]).wait()
        rows = xr[j].reshape(512, 128)

        def group(g, inner):
            parts = []
            for i in range(4):
                top = cr[j, g, i]
                parts.append(jnp.concatenate([top, pltpu.roll(top, 64, 1) * sign], axis=0))
            prod = dot(rows, jnp.concatenate(parts, axis=1))
            total = None
            for i in range(4):
                piece = prod[:, i * 128 : (i + 1) * 128].reshape(4, 16, 8, 128)
                term = piece * coef[g * 4 + i].reshape(4, 1, 8, 128)
                total = term if total is None else total + term
            total = total.reshape(32, 16, 128)

            @pl.when(g == 0)
            def _():
                ys[j] = total

            @pl.when(g > 0)
            def _():
                ys[j] += total

            return inner

        lax.fori_loop(0, 4, group, 0)

        def send_y(i, inner):
            d = jnp.where(i < 16, (i // 4) * 8 + 4 + i % 4, ((i - 15) // 4) * 8 + (i - 15) % 4)
            tz, tmy, tcol = plane(d - 1)
            pltpu.make_async_remote_copy(
                ys.at[j, tz * 8 + tcol], yr.at[l, j, kz], y_send, y_recv,
                device_id=(tz, tmy, tcol), device_id_type=MESH,
            ).start()
            return inner

        lax.fori_loop(0, 31, send_y, 0)
        pltpu.make_async_copy(ys.at[j, z * 8 + col], yr.at[l, j, kz], y_own).start()
        return carry

    lax.fori_loop(0, 4, mode_step, 0)
    pltpu.make_async_copy(ys.at[:, 0], ys.at[:, 0], y_own).wait()
    pltpu.make_async_copy(ys.at[:, 0:31], ys.at[:, 0:31], y_recv).wait()
    pltpu.make_async_copy(sr.at[0:3], sr.at[0:3], fac_send.at[0]).wait()
    pltpu.make_async_copy(sr.at[0:3], sr.at[0:3], fac_send.at[1]).wait()
    pltpu.make_async_copy(bs.at[0:15], bs.at[0:15], b_send).wait()
    pltpu.make_async_copy(xr.at[:, 0:30], xr.at[:, 0:30], x_send).wait()
    pltpu.make_async_copy(cs.at[:, 0:7], cs.at[:, 0:7], c_send).wait()
    pltpu.make_async_copy(ys.at[:, 0:31], ys.at[:, 0:31], y_send).wait()


def finish_kernel(modes_ref, fout_ref, out_ref):
    factor = fout_ref[...].T
    blank = jnp.zeros_like(factor)
    part = pl.program_id(0)
    left = jnp.where(part == 0, factor, blank)
    right = jnp.where(part == 0, blank, factor)
    wide = jnp.concatenate([left, right], axis=1)
    base = pl.program_id(1) * 8
    for k in range(8):
        modes = modes_ref[pl.ds(base + k, 128, stride=16), :]
        out_ref[pl.ds(k, 128, stride=8), :] = dot(wide, modes, ((1,), (1,)))


def per_device(
    spectrum, core_tensor, input_factor, output_factor, first_factor, second_factor, third_factor
):
    spec = spectrum.reshape(4096, 128)
    core = jnp.transpose(core_tensor[:, :, :, 0], (0, 1, 3, 4, 2)).reshape(2, 8, 256, 64)
    anywhere = pl.BlockSpec(memory_space=pl.ANY)
    vmem = lambda *shape: pltpu.VMEM(shape, F32)
    dma = pltpu.SemaphoreType.DMA
    values = pl.pallas_call(
        kernel,
        out_shape=jax.ShapeDtypeStruct((2, 4, 16, 16, 128), F32),
        in_specs=[anywhere] * 6,
        out_specs=anywhere,
        scratch_shapes=[
            vmem(4096, 128),
            vmem(2, 8, 256, 64),
            vmem(64, 128), vmem(64, 128), vmem(8, 16), vmem(8, 16), vmem(16, 16),
            vmem(2, 4, 16, 16, 128),
            vmem(4, 16, 16, 128),
            vmem(4, 32, 16, 128),
            vmem(16, 2, 4, 16, 128),
            vmem(2, 4, 4, 4, 16, 128),
            vmem(2, 8, 4, 4, 16, 128),
            vmem(4, 4, 4, 64, 128),
            vmem(4, 32, 16, 128),
            vmem(2, 8, 128),
            vmem(4, 8, 128),
            vmem(4, 8, 128),
            vmem(256, 256),
            vmem(256, 128),
            vmem(16, 32, 128),
            dma((6,)), dma((2,)), dma((2,)), dma, dma((2,)), dma, dma, dma, dma, dma, dma((4,)), dma, dma,
            dma,
        ],
        compiler_params=pltpu.CompilerParams(
            collective_id=0, has_side_effects=True, vmem_limit_bytes=63 * 1024 * 1024
        ),
    )(spec, core, input_factor.T, first_factor, second_factor, third_factor)
    out = pl.pallas_call(
        finish_kernel,
        grid=(2, 2),
        out_shape=jax.ShapeDtypeStruct((4096, 128), F32),
        in_specs=[
            pl.BlockSpec((2048, 128), lambda c, b: (0, 0)),
            pl.BlockSpec((64, 128), lambda c, b: (0, 0)),
        ],
        out_specs=pl.BlockSpec((1024, 128), lambda c, b: (c * 2 + b, 0)),
        compiler_params=pltpu.CompilerParams(vmem_limit_bytes=63 * 1024 * 1024),
    )(values.reshape(2048, 128), output_factor.T)
    return out.reshape(2, 2, 128, 8, 128)


def solution(mesh):
    placed = (
        P(None, "col", None, "mx", "my"),
        P(None, "col", None, ("mx", "my"), None, None),
        P(),
        P(),
        P("mx", None),
        P("my", None),
        P(),
    )
    return jax.shard_map(
        per_device,
        mesh=mesh,
        in_specs=placed,
        out_specs=P(None, "col", None, "mx", "my"),
        check_vma=False,
    )
```

```python
import jax
import jax.numpy as jnp
from jax import lax
from jax.experimental import pallas as pl
from jax.experimental.pallas import tpu as pltpu
from jax.sharding import PartitionSpec as P

MESH = pl.DeviceIdType.MESH
F32 = jnp.float32


def exact(a, b):
    return lax.dot_general(
        a, b, (((1,), (0,)), ((), ())), precision=lax.Precision.HIGHEST, preferred_element_type=F32
    )


def split(a):
    high = a.astype(jnp.bfloat16)
    return high, (a - high.astype(F32)).astype(jnp.bfloat16)


def dot(a, b, dims=((1,), (0,))):
    (ah, al), (bh, bl) = split(a), split(b)
    one = lambda u, v: lax.dot_general(u, v, (dims, ((), ())), preferred_element_type=F32)
    return one(ah, bh) + (one(al, bh) + one(ah, bl))


def iota(shape, dim):
    return lax.broadcasted_iota(jnp.int32, shape, dim)


def kernel(
    spec_hbm, core_hbm, fin_hbm, first_hbm, second_hbm, third_hbm,
    yr,
    spec, core, fin_ref, fin, first_ref, second_ref, third_ref, xs, xp, xr, bs, br, cs, cr, ys, stage, fr, sr, m1, m2, coef,
    in_sem, fac_send, fac_recv, b_send, b_recv, p_send, p_recv, x_send, x_recv, c_send, c_recv, y_send, y_recv, y_own,
):
    z, my, col = lax.axis_index("mx"), lax.axis_index("my"), lax.axis_index("col")
    h, e = my // 2, my % 2
    l, x = col // 4, col % 4
    kz = z * 4 + x

    loads = [
        pltpu.make_async_copy(far, here, in_sem.at[n])
        for n, (far, here) in enumerate((
            (fin_hbm, fin_ref),
            (spec_hbm.at[:, 0], spec.at[:, 0]),
            (spec_hbm.at[:, 1], spec.at[:, 1]),
            (first_hbm, first_ref), (second_hbm, second_ref), (third_hbm, third_ref),
            (core_hbm, core),
        ))
    ]
    for load in loads:
        load.start()

    def plane(i):
        d = i + 1
        return (z + d // 8) % 4, my, ((l + (d // 4) % 2) % 2) * 4 + (x + d % 4) % 4

    def square(i):
        d = i + 1
        return z, ((h + d // 4) % 2) * 2 + (e + d % 2) % 2, ((l + (d // 2) % 2) % 2) * 4 + x

    barrier = pltpu.get_barrier_semaphore()

    def greet_plane(i, carry):
        pl.semaphore_signal(barrier, inc=1, device_id=plane(i), device_id_type=MESH)
        return carry

    def greet_square(i, carry):
        d = i + jnp.where(i >= 1, 1, 0)
        pl.semaphore_signal(barrier, inc=1, device_id=square(d), device_id_type=MESH)
        return carry

    lax.fori_loop(0, 31, greet_plane, 0)
    lax.fori_loop(0, 6, greet_square, 0)

    loads[0].wait()
    for a in range(16):
        true = (a // 8) * 32 + (a % 4) * 8 + (a // 4 % 2) * 4
        fin[4 * a : 4 * a + 4, :] = fin_ref[true : true + 4, :]
    xs2 = xs.reshape(2048, 128)

    def project(b):
        loads[1 + b].wait()

        def step(n, carry):
            for k in range(4):
                k = n * 4 + k
                real = dot(fin[...], spec[0, b, pl.ds(k, 128, stride=8), :])
                imag = dot(fin[...], spec[1, b, pl.ds(k, 128, stride=8), :])
                both = jnp.concatenate([real, imag], axis=0).T
                xs2[pl.ds(b * 8 + k, 128, stride=16), :] = both
            return carry

        lax.fori_loop(0, 2, step, 0)

    def swap(b):
        half = pl.ds(b * 8, 8)
        return pltpu.make_async_remote_copy(
            xs.at[1 - l, :, :, half], xp.at[:, :, half], p_send.at[b], p_recv.at[b],
            device_id=(z, my, (1 - l) * 4 + x), device_id_type=MESH,
        )

    project(0)
    pl.semaphore_wait(barrier, 37)
    swap(0).start()
    project(1)
    swap(1).start()

    for load in loads[3:6]:
        load.wait()
    stage[...] = jnp.zeros_like(stage)
    stage[0, :, 0:16] = first_ref[...]
    stage[1, :, 0:16] = second_ref[...]
    fr[pl.ds(z, 1)] = stage[0:1]
    sr[pl.ds(my, 1)] = stage[1:2]

    def send_first(i, carry):
        pltpu.make_async_remote_copy(
            stage.at[0], fr.at[z], fac_send.at[0], fac_recv.at[0],
            device_id=((z + i + 1) % 4, my, col), device_id_type=MESH,
        ).start()
        d = i + 1
        pltpu.make_async_remote_copy(
            stage.at[1], sr.at[my], fac_send.at[1], fac_recv.at[1],
            device_id=(z, ((h + d // 2) % 2) * 2 + (e + d % 2) % 2, col), device_id_type=MESH,
        ).start()
        return carry

    lax.fori_loop(0, 3, send_first, 0)

    spread = jnp.where(iota((16, 256), 1) % 16 == iota((16, 256), 0), 1.0, 0.0)
    wide = exact(third_ref[...], spread)
    wide = jnp.broadcast_to(wide[:, None, :], (16, 16, 256)).reshape(256, 256)
    m1[...] = jnp.where(iota((256, 256), 0) % 16 == iota((256, 256), 1) // 16, wide, 0.0)
    loads[6].wait()

    def first_exchange(half, carry):
        for p in range(4):
            both = jnp.concatenate([core[0, half * 4 + p], core[1, half * 4 + p]], axis=1)
            bs[:, half, p] = dot(m1[...], both).reshape(16, 16, 128)

        def send_b(i, inner):
            d = i + 1
            tz, tx = (z + d // 4) % 4, (x + d % 4) % 4
            pltpu.make_async_remote_copy(
                bs.at[tz * 4 + tx, half], br.at[half, z, x], b_send, b_recv.at[half],
                device_id=(tz, my, l * 4 + tx), device_id_type=MESH,
            ).start()
            return inner

        lax.fori_loop(0, 15, send_b, 0)
        br[half, z, x] = bs[kz, half]
        return carry

    lax.fori_loop(0, 2, first_exchange, 0)

    pltpu.make_async_copy(sr.at[0:3], sr.at[0:3], fac_recv.at[1]).wait()
    spread2 = jnp.where(iota((128, 128), 1) % 16 == iota((128, 128), 0), 1.0, 0.0)
    wide2 = exact(sr[...].reshape(32, 128), spread2)
    wide2 = jnp.broadcast_to(wide2[:, None, :], (32, 8, 128)).reshape(256, 128)
    m2[...] = jnp.where(iota((256, 128), 0) % 8 == iota((256, 128), 1) // 16, wide2, 0.0)

    def send_x(source, sample):
        def step(i, carry):
            d = i + 1
            tz, tx = (z + d // 4) % 4, (x + d % 4) % 4
            pltpu.make_async_remote_copy(
                source.at[:, tz * 4 + tx], xr.at[:, sample], x_send, x_recv,
                device_id=(tz, my, l * 4 + tx), device_id_type=MESH,
            ).start()
            return carry

        lax.fori_loop(0, 15, step, 0)
        for j in range(4):
            xr[j, sample] = source[j, kz]

    for half in range(2):
        pltpu.make_async_copy(bs.at[0:15, 0], bs.at[0:15, 0], b_recv.at[half]).wait()
        if half == 1:
            send_x(xs.at[l], z * 8 + col)

        def second_step(n, carry, half=half):
            for i in range(4):
                zs, pair = n * 2 + i // 2, i % 2
                block = br[half, zs, pl.ds(pair * 2, 2)].reshape(128, 128)
                part = dot(m2[...], block).reshape(8, 4, 8, 128)
                cs[half, :, :, zs, pl.ds(pair * 8, 8), :] = part
            return carry

        lax.fori_loop(0, 2, second_step, 0)

        def send_c(n, carry, half=half):
            j, i = n // 7, n % 7
            tz, tmy, tcol = square(i)
            pltpu.make_async_remote_copy(
                cs.at[half, tmy * 2 + tcol // 4, j],
                cr.at[j, :, my, pl.ds(l * 32 + half * 16, 16), :],
                c_send, c_recv.at[j],
                device_id=(tz, tmy, tcol), device_id_type=MESH,
            ).start()
            return carry

        lax.fori_loop(0, 28, send_c, 0)

        def keep_c(n, carry, half=half):
            j, zs = n // 4, n % 4
            cr[j, zs, my, pl.ds(l * 32 + half * 16, 16), :] = cs[half, my * 2 + l, j, zs]
            return carry

        lax.fori_loop(0, 16, keep_c, 0)

    swap(0).wait()
    swap(1).wait()
    send_x(xp, z * 8 + (1 - l) * 4 + x)

    pltpu.make_async_copy(sr.at[0:3], sr.at[0:3], fac_recv.at[0]).wait()
    for s in range(16):
        coef[s] = jnp.broadcast_to(fr[...].reshape(32, 128)[:, s : s + 1], (32, 128))
    pltpu.make_async_copy(xr.at[:, 0:30], xr.at[:, 0:30], x_recv).wait()

    sign = jnp.where(iota((64, 128), 1) < 64, -1.0, 1.0)

    def mode_step(j, carry):
        pltpu.make_async_copy(cs.at[:, 0:7, 0], cs.at[:, 0:7, 0], c_recv.at[j]).wait()
        rows = xr[j].reshape(512, 128)

        def group(g, inner):
            parts = []
            for i in range(4):
                top = cr[j, g, i]
                parts.append(jnp.concatenate([top, pltpu.roll(top, 64, 1) * sign], axis=0))
            prod = dot(rows, jnp.concatenate(parts, axis=1))
            total = None
            for i in range(4):
                piece = prod[:, i * 128 : (i + 1) * 128].reshape(4, 16, 8, 128)
                term = piece * coef[g * 4 + i].reshape(4, 1, 8, 128)
                total = term if total is None else total + term
            total = total.reshape(32, 16, 128)

            @pl.when(g == 0)
            def _():
                ys[j] = total

            @pl.when(g > 0)
            def _():
                ys[j] += total

            return inner

        lax.fori_loop(0, 4, group, 0)

        def send_y(i, inner):
            d = jnp.where(i < 16, (i // 4) * 8 + 4 + i % 4, ((i - 15) // 4) * 8 + (i - 15) % 4)
            tz, tmy, tcol = plane(d - 1)
            pltpu.make_async_remote_copy(
                ys.at[j, tz * 8 + tcol], yr.at[l, j, kz], y_send, y_recv,
                device_id=(tz, tmy, tcol), device_id_type=MESH,
            ).start()
            return inner

        lax.fori_loop(0, 31, send_y, 0)
        pltpu.make_async_copy(ys.at[j, z * 8 + col], yr.at[l, j, kz], y_own).start()
        return carry

    lax.fori_loop(0, 4, mode_step, 0)
    pltpu.make_async_copy(ys.at[:, 0], ys.at[:, 0], y_own).wait()
    pltpu.make_async_copy(ys.at[:, 0:31], ys.at[:, 0:31], y_recv).wait()
    pltpu.make_async_copy(sr.at[0:3], sr.at[0:3], fac_send.at[0]).wait()
    pltpu.make_async_copy(sr.at[0:3], sr.at[0:3], fac_send.at[1]).wait()
    pltpu.make_async_copy(bs.at[0:15], bs.at[0:15], b_send).wait()
    pltpu.make_async_copy(xr.at[:, 0:30], xr.at[:, 0:30], x_send).wait()
    pltpu.make_async_copy(cs.at[:, 0:7], cs.at[:, 0:7], c_send).wait()
    pltpu.make_async_copy(ys.at[:, 0:31], ys.at[:, 0:31], y_send).wait()


def finish_kernel(modes_ref, fout_ref, out_ref):
    factor = fout_ref[...].T
    blank = jnp.zeros_like(factor)
    wide = jnp.concatenate(
        [jnp.concatenate([factor, blank], axis=1), jnp.concatenate([blank, factor], axis=1)], axis=0
    )
    modes = modes_ref.reshape(1024, 128)
    for k in range(8):
        mixed = dot(wide, modes[pl.ds(k, 128, stride=8), :], ((1,), (1,)))
        out_ref[0, 0, pl.ds(k, 128, stride=8), :] = mixed[0:128]
        out_ref[1, 0, pl.ds(k, 128, stride=8), :] = mixed[128:256]


def per_device(
    spectrum, core_tensor, input_factor, output_factor, first_factor, second_factor, third_factor
):
    spec = spectrum.reshape(2, 2, 1024, 128)
    core = jnp.transpose(core_tensor[:, :, :, 0], (0, 1, 3, 4, 2)).reshape(2, 8, 256, 64)
    anywhere = pl.BlockSpec(memory_space=pl.ANY)
    vmem = lambda *shape: pltpu.VMEM(shape, F32)
    dma = pltpu.SemaphoreType.DMA
    values = pl.pallas_call(
        kernel,
        out_shape=jax.ShapeDtypeStruct((2, 4, 16, 16, 128), F32),
        in_specs=[anywhere] * 6,
        out_specs=anywhere,
        scratch_shapes=[
            vmem(2, 2, 1024, 128),
            vmem(2, 8, 256, 64),
            vmem(64, 128), vmem(64, 128), vmem(8, 16), vmem(8, 16), vmem(16, 16),
            vmem(2, 4, 16, 16, 128),
            vmem(4, 16, 16, 128),
            vmem(4, 32, 16, 128),
            vmem(16, 2, 4, 16, 128),
            vmem(2, 4, 4, 4, 16, 128),
            vmem(2, 8, 4, 4, 16, 128),
            vmem(4, 4, 4, 64, 128),
            vmem(4, 32, 16, 128),
            vmem(2, 8, 128),
            vmem(4, 8, 128),
            vmem(4, 8, 128),
            vmem(256, 256),
            vmem(256, 128),
            vmem(16, 32, 128),
            dma((7,)), dma((2,)), dma((2,)), dma, dma((2,)), dma((2,)), dma((2,)), dma, dma, dma, dma((4,)), dma, dma,
            dma,
        ],
        compiler_params=pltpu.CompilerParams(
            collective_id=0, has_side_effects=True, vmem_limit_bytes=63 * 1024 * 1024
        ),
    )(spec, core, input_factor.T, first_factor, second_factor, third_factor)
    out = pl.pallas_call(
        finish_kernel,
        grid=(2,),
        out_shape=jax.ShapeDtypeStruct((2, 2, 1024, 128), F32),
        in_specs=[
            pl.BlockSpec((128, 1, 8, 128), lambda b: (0, b, 0, 0)),
            pl.BlockSpec((64, 128), lambda b: (0, 0)),
        ],
        out_specs=pl.BlockSpec((2, 1, 1024, 128), lambda b: (0, b, 0, 0)),
        compiler_params=pltpu.CompilerParams(vmem_limit_bytes=63 * 1024 * 1024),
    )(values.reshape(128, 2, 8, 128), output_factor.T)
    return out.reshape(2, 2, 128, 8, 128)


def solution(mesh):
    placed = (
        P(None, "col", None, "mx", "my"),
        P(None, "col", None, ("mx", "my"), None, None),
        P(),
        P(),
        P("mx", None),
        P("my", None),
        P(),
    )
    return jax.shard_map(
        per_device,
        mesh=mesh,
        in_specs=placed,
        out_specs=P(None, "col", None, "mx", "my"),
        check_vma=False,
    )
```

```python
import jax
import jax.numpy as jnp
from jax import lax
from jax.experimental import pallas as pl
from jax.experimental.pallas import tpu as pltpu
from jax.sharding import PartitionSpec as P

MESH = pl.DeviceIdType.MESH
F32 = jnp.float32


def exact(a, b):
    return lax.dot_general(
        a, b, (((1,), (0,)), ((), ())), precision=lax.Precision.HIGHEST, preferred_element_type=F32
    )


def split(a):
    high = a.astype(jnp.bfloat16)
    return high, (a - high.astype(F32)).astype(jnp.bfloat16)


def dot(a, b, dims=((1,), (0,))):
    (ah, al), (bh, bl) = split(a), split(b)
    one = lambda u, v: lax.dot_general(u, v, (dims, ((), ())), preferred_element_type=F32)
    return one(ah, bh) + (one(al, bh) + one(ah, bl))


def iota(shape, dim):
    return lax.broadcasted_iota(jnp.int32, shape, dim)


def kernel(
    spec_hbm, core_hbm, fin_hbm, first_hbm, second_hbm, third_hbm,
    yr,
    spec, core, fin_ref, fin, first_ref, second_ref, third_ref, xs, xp, xr, bs, br, cs, cr, ys, stage, fr, sr, m1, m2, coef,
    in_sem, fac_send, fac_recv, b_send, b_recv, p_send, p_recv, x_send, x_recv, c_send, c_recv, y_send, y_recv, y_own,
):
    z, my, col = lax.axis_index("mx"), lax.axis_index("my"), lax.axis_index("col")
    h, e = my // 2, my % 2
    l, x = col // 4, col % 4
    kz = z * 4 + x

    loads = [
        pltpu.make_async_copy(far, here, in_sem.at[n])
        for n, (far, here) in enumerate((
            (fin_hbm, fin_ref),
            (spec_hbm.at[:, 0], spec.at[:, 0]),
            (spec_hbm.at[:, 1], spec.at[:, 1]),
            (first_hbm, first_ref), (second_hbm, second_ref), (third_hbm, third_ref),
            (core_hbm.at[:, 0:4], core.at[:, 0:4]),
            (core_hbm.at[:, 4:8], core.at[:, 4:8]),
        ))
    ]
    for n in (5, 6, 0, 1, 3, 4, 7, 2):
        loads[n].start()

    rem, div = lax.rem, lax.div

    def plane(i):
        d = jnp.int32(i + 1)
        return rem(z + div(d, 8), 4), my, rem(l + rem(div(d, 4), 2), 2) * 4 + rem(x + rem(d, 4), 4)

    def square(i):
        d = jnp.int32(i + 1)
        return (
            z,
            rem(h + div(d, 4), 2) * 2 + rem(e + rem(d, 2), 2),
            rem(l + rem(div(d, 2), 2), 2) * 4 + x,
        )

    barrier = pltpu.get_barrier_semaphore()

    def hops(d):
        return (0, 1, 2, 1)[d // 8] + (d // 4) % 2 + (0, 1, 2, 1)[d % 4]

    for d in sorted(range(1, 32), key=lambda d: -hops(d)):
        pl.semaphore_signal(barrier, inc=1, device_id=plane(d - 1), device_id_type=MESH)
    for d in (4, 5, 6, 7, 3, 1):
        pl.semaphore_signal(barrier, inc=1, device_id=square(d - 1), device_id_type=MESH)

    loads[0].wait()
    for a in range(16):
        true = (a // 8) * 32 + (a % 4) * 8 + (a // 4 % 2) * 4
        fin[4 * a : 4 * a + 4, :] = fin_ref[true : true + 4, :]

    def project(b):
        loads[1 + b].wait()

        def step(n, carry):
            for k in range(4):
                k = n * 4 + k
                real = dot(fin[...], spec[0, b, pl.ds(k, 128, stride=8), :])
                imag = dot(fin[...], spec[1, b, pl.ds(k, 128, stride=8), :])
                both = jnp.concatenate([real, imag], axis=0).T
                for part in range(2):
                    rows = xs.at[part, b].reshape(512, 128)
                    rows[pl.ds(k, 64, stride=8), :] = both[part * 64 : part * 64 + 64]
            return carry

        lax.fori_loop(0, 2, step, 0)

    def swap(b):
        return pltpu.make_async_remote_copy(
            xs.at[1 - l, b], xp.at[b], p_send.at[b], p_recv.at[b],
            device_id=(z, my, (1 - l) * 4 + x), device_id_type=MESH,
        )

    for load in loads[3:5]:
        load.wait()
    stage[...] = jnp.zeros_like(stage)
    stage[0, :, 0:16] = first_ref[...]
    stage[1, :, 0:16] = second_ref[...]
    fr[pl.ds(z, 1)] = stage[0:1]
    sr[pl.ds(my, 1)] = stage[1:2]

    loads[5].wait()
    spread = jnp.where(iota((16, 256), 1) % 16 == iota((16, 256), 0), 1.0, 0.0)
    wide = exact(third_ref[...], spread)
    wide = jnp.broadcast_to(wide[:, None, :], (16, 16, 256)).reshape(256, 256)
    m1[...] = jnp.where(iota((256, 256), 0) % 16 == iota((256, 256), 1) // 16, wide, 0.0)

    def third_step(half):
        loads[6 + half].wait()
        for p in range(4):
            both = jnp.concatenate([core[0, half * 4 + p], core[1, half * 4 + p]], axis=1)
            bs[:, half, p] = dot(m1[...], both).reshape(16, 16, 128)

    def send_b(half):
        def step(i, carry):
            d = i + 1
            tz, tx = lax.rem(z + lax.div(d, 4), 4), lax.rem(x + lax.rem(d, 4), 4)
            pltpu.make_async_remote_copy(
                bs.at[tz * 4 + tx, half], br.at[half, z, x], b_send, b_recv.at[half],
                device_id=(tz, my, l * 4 + tx), device_id_type=MESH,
            ).start()
            return carry

        lax.fori_loop(0, 15, step, 0)
        br[half, z, x] = bs[kz, half]

    third_step(0)
    project(0)
    pl.semaphore_wait(barrier, 37)
    swap(0).start()
    send_b(0)
    third_step(1)
    send_b(1)
    project(1)
    swap(1).start()

    def send_first(i, carry):
        pltpu.make_async_remote_copy(
            stage.at[0], fr.at[z], fac_send.at[0], fac_recv.at[0],
            device_id=((z + i + 1) % 4, my, col), device_id_type=MESH,
        ).start()
        d = i + 1
        pltpu.make_async_remote_copy(
            stage.at[1], sr.at[my], fac_send.at[1], fac_recv.at[1],
            device_id=(z, ((h + d // 2) % 2) * 2 + (e + d % 2) % 2, col), device_id_type=MESH,
        ).start()
        return carry

    lax.fori_loop(0, 3, send_first, 0)

    pltpu.make_async_copy(sr.at[0:3], sr.at[0:3], fac_recv.at[1]).wait()
    spread2 = jnp.where(iota((128, 128), 1) % 16 == iota((128, 128), 0), 1.0, 0.0)
    wide2 = exact(sr[...].reshape(32, 128), spread2)
    wide2 = jnp.broadcast_to(wide2[:, None, :], (32, 8, 128)).reshape(256, 128)
    m2[...] = jnp.where(iota((256, 128), 0) % 8 == iota((256, 128), 1) // 16, wide2, 0.0)

    def send_x(source, sample):
        def step(i, carry):
            d = i + 1
            tz, tx = (z + d // 4) % 4, (x + d % 4) % 4
            pltpu.make_async_remote_copy(
                source.at[:, :, tz * 4 + tx], xr.at[:, :, sample], x_send, x_recv,
                device_id=(tz, my, l * 4 + tx), device_id_type=MESH,
            ).start()
            return carry

        lax.fori_loop(0, 15, step, 0)
        for b in range(2):
            for j in range(4):
                xr[b, j, sample] = source[b, j, kz]

    for half in range(2):
        pltpu.make_async_copy(bs.at[0:15, 0], bs.at[0:15, 0], b_recv.at[half]).wait()
        if half == 1:
            send_x(xs.at[l], z * 8 + col)

        def second_step(n, carry, half=half):
            for i in range(4):
                zs, pair = n * 2 + i // 2, i % 2
                block = br[half, zs, pl.ds(pair * 2, 2)].reshape(128, 128)
                part = dot(m2[...], block).reshape(8, 4, 8, 128)
                cs[half, :, :, zs, pl.ds(pair * 8, 8), :] = part
            return carry

        lax.fori_loop(0, 2, second_step, 0)

        def send_c(n, carry, half=half):
            j, i = n // 7, n % 7
            tz, tmy, tcol = square(i)
            pltpu.make_async_remote_copy(
                cs.at[half, tmy * 2 + tcol // 4, j],
                cr.at[j, my, l, half],
                c_send, c_recv.at[j],
                device_id=(tz, tmy, tcol), device_id_type=MESH,
            ).start()
            return carry

        lax.fori_loop(0, 28, send_c, 0)

        def keep_c(n, carry, half=half):
            j, zs = n // 4, n % 4
            cr[j, my, l, half, zs] = cs[half, my * 2 + l, j, zs]
            return carry

        lax.fori_loop(0, 16, keep_c, 0)

    swap(0).wait()
    swap(1).wait()
    send_x(xp, z * 8 + (1 - l) * 4 + x)

    pltpu.make_async_copy(sr.at[0:3], sr.at[0:3], fac_recv.at[0]).wait()
    for s in range(16):
        coef[s] = jnp.broadcast_to(fr[...].reshape(32, 128)[:, s : s + 1], (32, 128))
    pltpu.make_async_copy(xr.at[:, :, 0:30], xr.at[:, :, 0:30], x_recv).wait()

    sign = jnp.where(iota((64, 128), 1) < 64, -1.0, 1.0)

    def mode_step(j, carry):
        pltpu.make_async_copy(cs.at[:, 0:7, 0], cs.at[:, 0:7, 0], c_recv.at[j]).wait()
        high, low = split(xr[:, j].reshape(512, 128))
        both = jnp.concatenate([high, low], axis=1)

        def group(g):
            parts = []
            for i in range(4):
                top = cr[j, i, :, :, g].reshape(64, 128)
                parts.append(jnp.concatenate([top, pltpu.roll(top, 64, 1) * sign], axis=0))
            upper, lower = split(jnp.concatenate(parts, axis=1))
            twice = jnp.concatenate([upper, upper], axis=0)
            one = lambda u, v: lax.dot_general(
                u, v, (((1,), (0,)), ((), ())), preferred_element_type=F32
            )
            prod = one(both, twice) + one(high, lower)
            total = None
            for i in range(4):
                piece = prod[:, i * 128 : (i + 1) * 128].reshape(2, 4, 8, 8, 128)
                term = piece * coef[g * 4 + i].reshape(1, 4, 1, 8, 128)
                total = term if total is None else total + term
            return total.reshape(2, 32, 8, 128)

        for g in range(4):
            total = group(g)
            for b in range(2):
                if g == 0:
                    ys[j, :, b] = total[b]
                else:
                    ys[j, :, b] += total[b]

        def send_y(i, inner):
            d = jnp.where(i < 16, (i // 4) * 8 + 4 + i % 4, ((i - 15) // 4) * 8 + (i - 15) % 4)
            tz, tmy, tcol = plane(d - 1)
            pltpu.make_async_remote_copy(
                ys.at[j, tz * 8 + tcol], yr.at[l, j, kz], y_send, y_recv,
                device_id=(tz, tmy, tcol), device_id_type=MESH,
            ).start()
            return inner

        lax.fori_loop(0, 31, send_y, 0)
        pltpu.make_async_copy(ys.at[j, z * 8 + col], yr.at[l, j, kz], y_own).start()
        return carry

    lax.fori_loop(0, 4, mode_step, 0)
    pltpu.make_async_copy(ys.at[:, 0], ys.at[:, 0], y_own).wait()
    pltpu.make_async_copy(ys.at[:, 0:31], ys.at[:, 0:31], y_recv).wait()
    pltpu.make_async_copy(sr.at[0:3], sr.at[0:3], fac_send.at[0]).wait()
    pltpu.make_async_copy(sr.at[0:3], sr.at[0:3], fac_send.at[1]).wait()
    pltpu.make_async_copy(bs.at[0:15], bs.at[0:15], b_send).wait()
    pltpu.make_async_copy(xr.at[:, :, 0:30], xr.at[:, :, 0:30], x_send).wait()
    pltpu.make_async_copy(cs.at[:, 0:7], cs.at[:, 0:7], c_send).wait()
    pltpu.make_async_copy(ys.at[:, 0:31], ys.at[:, 0:31], y_send).wait()


def finish_kernel(modes_ref, fout_ref, out_ref):
    factor = fout_ref[...].T
    blank = jnp.zeros_like(factor)
    wide = jnp.concatenate(
        [jnp.concatenate([factor, blank], axis=1), jnp.concatenate([blank, factor], axis=1)], axis=0
    )
    modes = modes_ref.reshape(1024, 128)
    for k in range(8):
        mixed = dot(wide, modes[pl.ds(k, 128, stride=8), :], ((1,), (1,)))
        out_ref[0, 0, pl.ds(k, 128, stride=8), :] = mixed[0:128]
        out_ref[1, 0, pl.ds(k, 128, stride=8), :] = mixed[128:256]


def per_device(
    spectrum, core_tensor, input_factor, output_factor, first_factor, second_factor, third_factor
):
    spec = spectrum.reshape(2, 2, 1024, 128)
    core = jnp.transpose(core_tensor[:, :, :, 0], (0, 1, 3, 4, 2)).reshape(2, 8, 256, 64)
    anywhere = pl.BlockSpec(memory_space=pl.ANY)
    vmem = lambda *shape: pltpu.VMEM(shape, F32)
    dma = pltpu.SemaphoreType.DMA
    values = pl.pallas_call(
        kernel,
        out_shape=jax.ShapeDtypeStruct((2, 4, 16, 2, 8, 128), F32),
        in_specs=[anywhere] * 6,
        out_specs=anywhere,
        scratch_shapes=[
            vmem(2, 2, 1024, 128),
            vmem(2, 8, 256, 64),
            vmem(64, 128), vmem(64, 128), vmem(8, 16), vmem(8, 16), vmem(16, 16),
            vmem(2, 2, 4, 16, 8, 128),
            vmem(2, 4, 16, 8, 128),
            vmem(2, 4, 32, 8, 128),
            vmem(16, 2, 4, 16, 128),
            vmem(2, 4, 4, 4, 16, 128),
            vmem(2, 8, 4, 4, 16, 128),
            vmem(4, 4, 2, 2, 4, 16, 128),
            vmem(4, 32, 2, 8, 128),
            vmem(2, 8, 128),
            vmem(4, 8, 128),
            vmem(4, 8, 128),
            vmem(256, 256),
            vmem(256, 128),
            vmem(16, 32, 128),
            dma((8,)), dma((2,)), dma((2,)), dma, dma((2,)), dma((2,)), dma((2,)), dma, dma, dma, dma((4,)), dma, dma,
            dma,
        ],
        compiler_params=pltpu.CompilerParams(
            collective_id=0, has_side_effects=True, vmem_limit_bytes=63 * 1024 * 1024
        ),
    )(spec, core, input_factor.T, first_factor, second_factor, third_factor)
    out = pl.pallas_call(
        finish_kernel,
        grid=(2,),
        out_shape=jax.ShapeDtypeStruct((2, 2, 1024, 128), F32),
        in_specs=[
            pl.BlockSpec((128, 1, 8, 128), lambda b: (0, b, 0, 0)),
            pl.BlockSpec((64, 128), lambda b: (0, 0)),
        ],
        out_specs=pl.BlockSpec((2, 1, 1024, 128), lambda b: (0, b, 0, 0)),
        compiler_params=pltpu.CompilerParams(vmem_limit_bytes=63 * 1024 * 1024),
    )(values.reshape(128, 2, 8, 128), output_factor.T)
    return out.reshape(2, 2, 128, 8, 128)


def solution(mesh):
    placed = (
        P(None, "col", None, "mx", "my"),
        P(None, "col", None, ("mx", "my"), None, None),
        P(),
        P(),
        P("mx", None),
        P("my", None),
        P(),
    )
    return jax.shard_map(
        per_device,
        mesh=mesh,
        in_specs=placed,
        out_specs=P(None, "col", None, "mx", "my"),
        check_vma=False,
    )
```

```python
import jax
import jax.numpy as jnp
from jax import lax
from jax.experimental import pallas as pl
from jax.experimental.pallas import tpu as pltpu
from jax.sharding import PartitionSpec as P

MESH = pl.DeviceIdType.MESH
F32 = jnp.float32


def exact(a, b):
    return lax.dot_general(
        a, b, (((1,), (0,)), ((), ())), precision=lax.Precision.HIGHEST, preferred_element_type=F32
    )


def split(a):
    high = a.astype(jnp.bfloat16)
    return high, (a - high.astype(F32)).astype(jnp.bfloat16)


def dot(a, b, dims=((1,), (0,))):
    (ah, al), (bh, bl) = split(a), split(b)
    one = lambda u, v: lax.dot_general(u, v, (dims, ((), ())), preferred_element_type=F32)
    return one(ah, bh) + (one(al, bh) + one(ah, bl))


def iota(shape, dim):
    return lax.broadcasted_iota(jnp.int32, shape, dim)


def kernel(
    spec_hbm, core_hbm, fin_hbm, first_hbm, second_hbm, third_hbm,
    yr,
    spec, core, fin_ref, fin, first_ref, second_ref, third_ref, xs, xp, xr, bs, br, cs, cr, ys, stage, fr, sr, m1, m2, coef,
    in_sem, fac_send, fac_recv, b_send, b_recv, p_send, p_recv, x_send, x_recv, c_send, c_recv, y_send, y_recv, y_own,
):
    z, my, col = lax.axis_index("mx"), lax.axis_index("my"), lax.axis_index("col")
    h, e = my // 2, my % 2
    l, x = col // 4, col % 4
    kz = z * 4 + x

    loads = [
        pltpu.make_async_copy(far, here, in_sem.at[n])
        for n, (far, here) in enumerate((
            (fin_hbm, fin_ref),
            (spec_hbm.at[:, 0], spec.at[:, 0]),
            (spec_hbm.at[:, 1], spec.at[:, 1]),
            (first_hbm, first_ref), (second_hbm, second_ref), (third_hbm, third_ref),
            (core_hbm.at[:, 0:4], core.at[:, 0:4]),
            (core_hbm.at[:, 4:8], core.at[:, 4:8]),
        ))
    ]
    for n in (5, 6, 0, 1, 3, 4, 7, 2):
        loads[n].start()

    rem, div = lax.rem, lax.div

    def plane(i):
        d = jnp.int32(i + 1)
        return rem(z + div(d, 8), 4), my, rem(l + rem(div(d, 4), 2), 2) * 4 + rem(x + rem(d, 4), 4)

    def square(i):
        d = jnp.int32(i + 1)
        return (
            z,
            rem(h + div(d, 4), 2) * 2 + rem(e + rem(d, 2), 2),
            rem(l + rem(div(d, 2), 2), 2) * 4 + x,
        )

    barrier = pltpu.get_barrier_semaphore()

    def hops(d):
        return (0, 1, 2, 1)[d // 8] + (d // 4) % 2 + (0, 1, 2, 1)[d % 4]

    for d in sorted([d for d in range(1, 32) if d // 4 % 2 == 0 or d == 4], key=lambda d: -hops(d)):
        pl.semaphore_signal(barrier, inc=1, device_id=plane(d - 1), device_id_type=MESH)
    for d in (4, 5, 6, 7, 3, 1):
        pl.semaphore_signal(barrier, inc=1, device_id=square(d - 1), device_id_type=MESH)

    loads[0].wait()
    for a in range(16):
        true = (a // 8) * 32 + (a % 4) * 8 + (a // 4 % 2) * 4
        fin[4 * a : 4 * a + 4, :] = fin_ref[true : true + 4, :]

    def project(b):
        loads[1 + b].wait()

        def step(n, carry):
            for k in range(4):
                k = n * 4 + k
                real = dot(fin[...], spec[0, b, pl.ds(k, 128, stride=8), :])
                imag = dot(fin[...], spec[1, b, pl.ds(k, 128, stride=8), :])
                both = jnp.concatenate([real, imag], axis=0).T
                for part in range(2):
                    rows = xs.at[part, b].reshape(512, 128)
                    rows[pl.ds(k, 64, stride=8), :] = both[part * 64 : part * 64 + 64]
            return carry

        lax.fori_loop(0, 2, step, 0)

    def swap(b):
        return pltpu.make_async_remote_copy(
            xs.at[1 - l, b], xp.at[b], p_send.at[b], p_recv.at[b],
            device_id=(z, my, (1 - l) * 4 + x), device_id_type=MESH,
        )

    for load in loads[3:5]:
        load.wait()
    stage[...] = jnp.zeros_like(stage)
    stage[0, :, 0:16] = first_ref[...]
    stage[1, :, 0:16] = second_ref[...]
    fr[pl.ds(z, 1)] = stage[0:1]
    sr[pl.ds(my, 1)] = stage[1:2]

    loads[5].wait()
    spread = jnp.where(iota((16, 256), 1) % 16 == iota((16, 256), 0), 1.0, 0.0)
    wide = exact(third_ref[...], spread)
    wide = jnp.broadcast_to(wide[:, None, :], (16, 16, 256)).reshape(256, 256)
    m1[...] = jnp.where(iota((256, 256), 0) % 16 == iota((256, 256), 1) // 16, wide, 0.0)

    def third_step(half):
        loads[6 + half].wait()
        for p in range(4):
            both = jnp.concatenate([core[0, half * 4 + p], core[1, half * 4 + p]], axis=1)
            bs[:, half, p] = dot(m1[...], both).reshape(16, 16, 128)

    def send_b(half):
        def step(i, carry):
            d = i + 1
            tz, tx = lax.rem(z + lax.div(d, 4), 4), lax.rem(x + lax.rem(d, 4), 4)
            pltpu.make_async_remote_copy(
                bs.at[tz * 4 + tx, half], br.at[half, z, x], b_send, b_recv.at[half],
                device_id=(tz, my, l * 4 + tx), device_id_type=MESH,
            ).start()
            return carry

        lax.fori_loop(0, 15, step, 0)
        br[half, z, x] = bs[kz, half]

    third_step(0)
    project(0)
    pl.semaphore_wait(barrier, 22)
    swap(0).start()
    send_b(0)
    third_step(1)
    send_b(1)
    project(1)
    swap(1).start()

    def send_first(i, carry):
        pltpu.make_async_remote_copy(
            stage.at[0], fr.at[z], fac_send.at[0], fac_recv.at[0],
            device_id=((z + i + 1) % 4, my, col), device_id_type=MESH,
        ).start()
        d = i + 1
        pltpu.make_async_remote_copy(
            stage.at[1], sr.at[my], fac_send.at[1], fac_recv.at[1],
            device_id=(z, ((h + d // 2) % 2) * 2 + (e + d % 2) % 2, col), device_id_type=MESH,
        ).start()
        return carry

    lax.fori_loop(0, 3, send_first, 0)

    pltpu.make_async_copy(sr.at[0:3], sr.at[0:3], fac_recv.at[1]).wait()
    spread2 = jnp.where(iota((128, 128), 1) % 16 == iota((128, 128), 0), 1.0, 0.0)
    wide2 = exact(sr[...].reshape(32, 128), spread2)
    wide2 = jnp.broadcast_to(wide2[:, None, :], (32, 8, 128)).reshape(256, 128)
    m2[...] = jnp.where(iota((256, 128), 0) % 8 == iota((256, 128), 1) // 16, wide2, 0.0)

    def send_x(source, sample):
        def step(i, carry):
            d = i + 1
            tz, tx = (z + d // 4) % 4, (x + d % 4) % 4
            pltpu.make_async_remote_copy(
                source.at[:, :, tz * 4 + tx], xr.at[:, :, sample], x_send, x_recv,
                device_id=(tz, my, l * 4 + tx), device_id_type=MESH,
            ).start()
            return carry

        lax.fori_loop(0, 15, step, 0)
        for b in range(2):
            for j in range(4):
                xr[b, j, sample] = source[b, j, kz]

    for half in range(2):
        pltpu.make_async_copy(bs.at[0:15, 0], bs.at[0:15, 0], b_recv.at[half]).wait()
        if half == 1:
            send_x(xs.at[l], z * 8 + col)

        def second_step(n, carry, half=half):
            for i in range(4):
                zs, pair = n * 2 + i // 2, i % 2
                block = br[half, zs, pl.ds(pair * 2, 2)].reshape(128, 128)
                part = dot(m2[...], block).reshape(8, 4, 8, 128)
                cs[half, :, :, zs, pl.ds(pair * 8, 8), :] = part
            return carry

        lax.fori_loop(0, 2, second_step, 0)

        def send_c(n, carry, half=half):
            j, i = n // 7, n % 7
            tz, tmy, tcol = square(i)
            pltpu.make_async_remote_copy(
                cs.at[half, tmy * 2 + tcol // 4, j],
                cr.at[j, my, l, half],
                c_send, c_recv.at[j],
                device_id=(tz, tmy, tcol), device_id_type=MESH,
            ).start()
            return carry

        lax.fori_loop(0, 28, send_c, 0)

        def keep_c(n, carry, half=half):
            j, zs = n // 4, n % 4
            cr[j, my, l, half, zs] = cs[half, my * 2 + l, j, zs]
            return carry

        lax.fori_loop(0, 16, keep_c, 0)

    swap(0).wait()
    swap(1).wait()
    send_x(xp, z * 8 + (1 - l) * 4 + x)

    pltpu.make_async_copy(sr.at[0:3], sr.at[0:3], fac_recv.at[0]).wait()
    for s in range(16):
        coef[s] = jnp.broadcast_to(fr[...].reshape(32, 128)[:, s : s + 1], (32, 128))
    pltpu.make_async_copy(xr.at[:, :, 0:30], xr.at[:, :, 0:30], x_recv).wait()

    sign = jnp.where(iota((64, 128), 1) < 64, -1.0, 1.0)

    def mode_step(j, carry):
        pltpu.make_async_copy(cs.at[:, 0:7, 0], cs.at[:, 0:7, 0], c_recv.at[j]).wait()
        high, low = split(xr[:, j].reshape(512, 128))
        both = jnp.concatenate([high, low], axis=1)

        def group(g):
            parts = []
            for i in range(4):
                top = cr[j, i, :, :, g].reshape(64, 128)
                parts.append(jnp.concatenate([top, pltpu.roll(top, 64, 1) * sign], axis=0))
            upper, lower = split(jnp.concatenate(parts, axis=1))
            twice = jnp.concatenate([upper, upper], axis=0)
            one = lambda u, v: lax.dot_general(
                u, v, (((1,), (0,)), ((), ())), preferred_element_type=F32
            )
            prod = one(both, twice) + one(high, lower)
            total = None
            for i in range(4):
                piece = prod[:, i * 128 : (i + 1) * 128].reshape(2, 4, 8, 8, 128)
                term = piece * coef[g * 4 + i].reshape(1, 4, 1, 8, 128)
                total = term if total is None else total + term
            return total.reshape(2, 32, 8, 128)

        for g in range(4):
            total = group(g)
            for b in range(2):
                if g == 0:
                    ys[j, :, b] = total[b]
                else:
                    ys[j, :, b] += total[b]

        def send_y(i, inner):
            d = jnp.where(i < 16, (i // 4) * 8 + 4 + i % 4, ((i - 15) // 4) * 8 + (i - 15) % 4)
            tz, tmy, tcol = plane(d - 1)
            pltpu.make_async_remote_copy(
                ys.at[j, tz * 8 + tcol], yr.at[l, j, kz], y_send, y_recv,
                device_id=(tz, tmy, tcol), device_id_type=MESH,
            ).start()
            return inner

        lax.fori_loop(0, 31, send_y, 0)
        pltpu.make_async_copy(ys.at[j, z * 8 + col], yr.at[l, j, kz], y_own).start()
        return carry

    lax.fori_loop(0, 4, mode_step, 0)
    pltpu.make_async_copy(ys.at[:, 0], ys.at[:, 0], y_own).wait()
    pltpu.make_async_copy(ys.at[:, 0:31], ys.at[:, 0:31], y_recv).wait()
    pltpu.make_async_copy(sr.at[0:3], sr.at[0:3], fac_send.at[0]).wait()
    pltpu.make_async_copy(sr.at[0:3], sr.at[0:3], fac_send.at[1]).wait()
    pltpu.make_async_copy(bs.at[0:15], bs.at[0:15], b_send).wait()
    pltpu.make_async_copy(xr.at[:, :, 0:30], xr.at[:, :, 0:30], x_send).wait()
    pltpu.make_async_copy(cs.at[:, 0:7], cs.at[:, 0:7], c_send).wait()
    pltpu.make_async_copy(ys.at[:, 0:31], ys.at[:, 0:31], y_send).wait()


def finish_kernel(modes_hbm, fout_hbm, out_hbm, modes_ref, fout_ref, out_ref, in_sem, out_sem):
    load_factor = pltpu.make_async_copy(fout_hbm, fout_ref, in_sem.at[2])
    loads = [
        pltpu.make_async_copy(modes_hbm.at[:, b], modes_ref.at[b], in_sem.at[b]) for b in range(2)
    ]
    load_factor.start()
    for load in loads:
        load.start()
    load_factor.wait()
    factor = fout_ref[...].T
    blank = jnp.zeros_like(factor)
    wide = jnp.concatenate(
        [jnp.concatenate([factor, blank], axis=1), jnp.concatenate([blank, factor], axis=1)], axis=0
    )
    stores = []
    for b in range(2):
        loads[b].wait()
        modes = modes_ref.at[b].reshape(1024, 128)
        for k in range(8):
            mixed = dot(wide, modes[pl.ds(k, 128, stride=8), :], ((1,), (1,)))
            out_ref[0, b, pl.ds(k, 128, stride=8), :] = mixed[0:128]
            out_ref[1, b, pl.ds(k, 128, stride=8), :] = mixed[128:256]
        store = pltpu.make_async_copy(out_ref.at[:, b], out_hbm.at[:, b], out_sem.at[b])
        store.start()
        stores.append(store)
    for store in stores:
        store.wait()


def per_device(
    spectrum, core_tensor, input_factor, output_factor, first_factor, second_factor, third_factor
):
    spec = spectrum.reshape(2, 2, 1024, 128)
    core = jnp.transpose(core_tensor[:, :, :, 0], (0, 1, 3, 4, 2)).reshape(2, 8, 256, 64)
    anywhere = pl.BlockSpec(memory_space=pl.ANY)
    vmem = lambda *shape: pltpu.VMEM(shape, F32)
    dma = pltpu.SemaphoreType.DMA
    values = pl.pallas_call(
        kernel,
        out_shape=jax.ShapeDtypeStruct((2, 4, 16, 2, 8, 128), F32),
        in_specs=[anywhere] * 6,
        out_specs=anywhere,
        scratch_shapes=[
            vmem(2, 2, 1024, 128),
            vmem(2, 8, 256, 64),
            vmem(64, 128), vmem(64, 128), vmem(8, 16), vmem(8, 16), vmem(16, 16),
            vmem(2, 2, 4, 16, 8, 128),
            vmem(2, 4, 16, 8, 128),
            vmem(2, 4, 32, 8, 128),
            vmem(16, 2, 4, 16, 128),
            vmem(2, 4, 4, 4, 16, 128),
            vmem(2, 8, 4, 4, 16, 128),
            vmem(4, 4, 2, 2, 4, 16, 128),
            vmem(4, 32, 2, 8, 128),
            vmem(2, 8, 128),
            vmem(4, 8, 128),
            vmem(4, 8, 128),
            vmem(256, 256),
            vmem(256, 128),
            vmem(16, 32, 128),
            dma((8,)), dma((2,)), dma((2,)), dma, dma((2,)), dma((2,)), dma((2,)), dma, dma, dma, dma((4,)), dma, dma,
            dma,
        ],
        compiler_params=pltpu.CompilerParams(
            collective_id=0, has_side_effects=True, vmem_limit_bytes=63 * 1024 * 1024
        ),
    )(spec, core, input_factor.T, first_factor, second_factor, third_factor)
    out = pl.pallas_call(
        finish_kernel,
        out_shape=jax.ShapeDtypeStruct((2, 2, 1024, 128), F32),
        in_specs=[anywhere, anywhere],
        out_specs=anywhere,
        scratch_shapes=[
            vmem(2, 128, 8, 128), vmem(64, 128), vmem(2, 2, 1024, 128), dma((3,)), dma((2,)),
        ],
        compiler_params=pltpu.CompilerParams(vmem_limit_bytes=63 * 1024 * 1024),
    )(values.reshape(128, 2, 8, 128), output_factor.T)
    return out.reshape(2, 2, 128, 8, 128)


def solution(mesh):
    placed = (
        P(None, "col", None, "mx", "my"),
        P(None, "col", None, ("mx", "my"), None, None),
        P(),
        P(),
        P("mx", None),
        P("my", None),
        P(),
    )
    return jax.shard_map(
        per_device,
        mesh=mesh,
        in_specs=placed,
        out_specs=P(None, "col", None, "mx", "my"),
        check_vma=False,
    )
```

```python
import jax
import jax.numpy as jnp
from jax import lax
from jax.experimental import pallas as pl
from jax.experimental.pallas import tpu as pltpu
from jax.sharding import PartitionSpec as P

MESH = pl.DeviceIdType.MESH
F32 = jnp.float32


def exact(a, b):
    return lax.dot_general(
        a, b, (((1,), (0,)), ((), ())), precision=lax.Precision.HIGHEST, preferred_element_type=F32
    )


def split(a):
    high = a.astype(jnp.bfloat16)
    return high, (a - high.astype(F32)).astype(jnp.bfloat16)


def dot(a, b, dims=((1,), (0,))):
    (ah, al), (bh, bl) = split(a), split(b)
    one = lambda u, v: lax.dot_general(u, v, (dims, ((), ())), preferred_element_type=F32)
    return one(ah, bh) + (one(al, bh) + one(ah, bl))


def iota(shape, dim):
    return lax.broadcasted_iota(jnp.int32, shape, dim)


def kernel(
    spec_hbm, core_hbm, fin_hbm, first_hbm, second_hbm, third_hbm,
    yr,
    spec, core, fin_ref, fin, first_ref, second_ref, third_ref, xs, xp, xr, bs, br, cs, cr, ys, stage, fr, sr, m1, m2, coef,
    in_sem, fac_send, fac_recv, b_send, b_recv, p_send, p_recv, x_send, x_recv, c_send, c_recv, y_send, y_recv, y_own,
):
    z, my, col = lax.axis_index("mx"), lax.axis_index("my"), lax.axis_index("col")
    h, e = my // 2, my % 2
    l, x = col // 4, col % 4
    kz = z * 4 + x

    loads = [
        pltpu.make_async_copy(far, here, in_sem.at[n])
        for n, (far, here) in enumerate((
            (fin_hbm, fin_ref),
            (spec_hbm.at[:, 0], spec.at[:, 0]),
            (spec_hbm.at[:, 1], spec.at[:, 1]),
            (first_hbm, first_ref), (second_hbm, second_ref), (third_hbm, third_ref),
            (core_hbm.at[:, 0:4], core.at[:, 0:4]),
            (core_hbm.at[:, 4:8], core.at[:, 4:8]),
        ))
    ]
    for n in (5, 6, 0, 1, 3, 4, 7, 2):
        loads[n].start()

    rem, div = lax.rem, lax.div

    def plane(i):
        d = jnp.int32(i + 1)
        return rem(z + div(d, 8), 4), my, rem(l + rem(div(d, 4), 2), 2) * 4 + rem(x + rem(d, 4), 4)

    def square(i):
        d = jnp.int32(i + 1)
        return (
            z,
            rem(h + div(d, 4), 2) * 2 + rem(e + rem(d, 2), 2),
            rem(l + rem(div(d, 2), 2), 2) * 4 + x,
        )

    barrier = pltpu.get_barrier_semaphore()

    def hops(d):
        return (0, 1, 2, 1)[d // 8] + (d // 4) % 2 + (0, 1, 2, 1)[d % 4]

    for d in sorted([d for d in range(1, 32) if d // 4 % 2 == 0 or d == 4], key=lambda d: -hops(d)):
        pl.semaphore_signal(barrier, inc=1, device_id=plane(d - 1), device_id_type=MESH)
    for d in (4, 5, 6, 7, 3, 1):
        pl.semaphore_signal(barrier, inc=1, device_id=square(d - 1), device_id_type=MESH)

    loads[0].wait()
    for a in range(16):
        true = (a // 8) * 32 + (a % 4) * 8 + (a // 4 % 2) * 4
        fin[4 * a : 4 * a + 4, :] = fin_ref[true : true + 4, :]

    def project(b):
        loads[1 + b].wait()

        def step(n, carry):
            for k in range(4):
                k = n * 4 + k
                real = dot(fin[...], spec[0, b, pl.ds(k, 128, stride=8), :])
                imag = dot(fin[...], spec[1, b, pl.ds(k, 128, stride=8), :])
                both = jnp.concatenate([real, imag], axis=0).T
                for part in range(2):
                    rows = xs.at[part, b].reshape(512, 128)
                    rows[pl.ds(k, 64, stride=8), :] = both[part * 64 : part * 64 + 64]
            return carry

        lax.fori_loop(0, 2, step, 0)

    def swap(b):
        return pltpu.make_async_remote_copy(
            xs.at[1 - l, b], xp.at[b], p_send.at[b], p_recv.at[b],
            device_id=(z, my, (1 - l) * 4 + x), device_id_type=MESH,
        )

    for load in loads[3:5]:
        load.wait()
    stage[...] = jnp.zeros_like(stage)
    stage[0, :, 0:16] = first_ref[...]
    stage[1, :, 0:16] = second_ref[...]
    fr[pl.ds(z, 1)] = stage[0:1]
    sr[pl.ds(my, 1)] = stage[1:2]

    loads[5].wait()
    spread = jnp.where(iota((16, 256), 1) % 16 == iota((16, 256), 0), 1.0, 0.0)
    wide = exact(third_ref[...], spread)
    wide = jnp.broadcast_to(wide[:, None, :], (16, 16, 256)).reshape(256, 256)
    m1[...] = jnp.where(iota((256, 256), 0) % 16 == iota((256, 256), 1) // 16, wide, 0.0)

    def third_step(half):
        loads[6 + half].wait()
        for p in range(4):
            both = jnp.concatenate([core[0, half * 4 + p], core[1, half * 4 + p]], axis=1)
            bs[:, half, p] = dot(m1[...], both).reshape(16, 16, 128)

    def send_b(half):
        def step(i, carry):
            d = i + 1
            tz, tx = lax.rem(z + lax.div(d, 4), 4), lax.rem(x + lax.rem(d, 4), 4)
            pltpu.make_async_remote_copy(
                bs.at[tz * 4 + tx, half], br.at[half, z, x], b_send, b_recv.at[half],
                device_id=(tz, my, l * 4 + tx), device_id_type=MESH,
            ).start()
            return carry

        lax.fori_loop(0, 15, step, 0)
        br[half, z, x] = bs[kz, half]

    third_step(0)
    project(0)
    pl.semaphore_wait(barrier, 22)
    swap(0).start()
    send_b(0)
    third_step(1)
    send_b(1)
    project(1)
    swap(1).start()

    def send_first(i, carry):
        pltpu.make_async_remote_copy(
            stage.at[0], fr.at[z], fac_send.at[0], fac_recv.at[0],
            device_id=((z + i + 1) % 4, my, col), device_id_type=MESH,
        ).start()
        d = i + 1
        pltpu.make_async_remote_copy(
            stage.at[1], sr.at[my], fac_send.at[1], fac_recv.at[1],
            device_id=(z, ((h + d // 2) % 2) * 2 + (e + d % 2) % 2, col), device_id_type=MESH,
        ).start()
        return carry

    lax.fori_loop(0, 3, send_first, 0)

    pltpu.make_async_copy(sr.at[0:3], sr.at[0:3], fac_recv.at[1]).wait()
    spread2 = jnp.where(iota((128, 128), 1) % 16 == iota((128, 128), 0), 1.0, 0.0)
    wide2 = exact(sr[...].reshape(32, 128), spread2)
    wide2 = jnp.broadcast_to(wide2[:, None, :], (32, 8, 128)).reshape(256, 128)
    m2[...] = jnp.where(iota((256, 128), 0) % 8 == iota((256, 128), 1) // 16, wide2, 0.0)

    def send_x(source, sample):
        def step(i, carry):
            d = i + 1
            tz, tx = (z + d // 4) % 4, (x + d % 4) % 4
            pltpu.make_async_remote_copy(
                source.at[:, :, tz * 4 + tx], xr.at[:, :, sample], x_send, x_recv,
                device_id=(tz, my, l * 4 + tx), device_id_type=MESH,
            ).start()
            return carry

        lax.fori_loop(0, 15, step, 0)
        for b in range(2):
            for j in range(4):
                xr[b, j, sample] = source[b, j, kz]

    for half in range(2):
        pltpu.make_async_copy(bs.at[0:15, 0], bs.at[0:15, 0], b_recv.at[half]).wait()
        if half == 1:
            send_x(xs.at[l], z * 8 + col)

        def second_step(n, carry, half=half):
            for i in range(4):
                zs, pair = n * 2 + i // 2, i % 2
                block = br[half, zs, pl.ds(pair * 2, 2)].reshape(128, 128)
                part = dot(m2[...], block).reshape(8, 4, 8, 128)
                cs[half, :, :, zs, pl.ds(pair * 8, 8), :] = part
            return carry

        lax.fori_loop(0, 2, second_step, 0)

        def send_c(j, carry, half=half):
            for d in (2, 3, 4, 5, 6, 7, 1):
                tz, tmy, tcol = square(d - 1)
                pltpu.make_async_remote_copy(
                    cs.at[half, tmy * 2 + lax.div(tcol, 4), j], cr.at[j, my, l, half],
                    c_send, c_recv.at[j],
                    device_id=(tz, tmy, tcol), device_id_type=MESH,
                ).start()
            return carry

        lax.fori_loop(0, 4, send_c, 0)

        def keep_c(n, carry, half=half):
            j, zs = n // 4, n % 4
            cr[j, my, l, half, zs] = cs[half, my * 2 + l, j, zs]
            return carry

        lax.fori_loop(0, 16, keep_c, 0)

    swap(0).wait()
    swap(1).wait()
    send_x(xp, z * 8 + (1 - l) * 4 + x)

    pltpu.make_async_copy(sr.at[0:3], sr.at[0:3], fac_recv.at[0]).wait()
    for s in range(16):
        coef[s] = jnp.broadcast_to(fr[...].reshape(32, 128)[:, s : s + 1], (32, 128))
    pltpu.make_async_copy(xr.at[:, :, 0:30], xr.at[:, :, 0:30], x_recv).wait()

    sign = jnp.where(iota((64, 128), 1) < 64, -1.0, 1.0)

    def mode_step(j, carry):
        pltpu.make_async_copy(cs.at[:, 0:7, 0], cs.at[:, 0:7, 0], c_recv.at[j]).wait()
        high, low = split(xr[:, j].reshape(512, 128))
        both = jnp.concatenate([high, low], axis=1)

        def group(g):
            parts = []
            for i in range(4):
                top = cr[j, i, :, :, g].reshape(64, 128)
                parts.append(jnp.concatenate([top, pltpu.roll(top, 64, 1) * sign], axis=0))
            upper, lower = split(jnp.concatenate(parts, axis=1))
            twice = jnp.concatenate([upper, upper], axis=0)
            one = lambda u, v: lax.dot_general(
                u, v, (((1,), (0,)), ((), ())), preferred_element_type=F32
            )
            prod = one(both, twice) + one(high, lower)
            total = None
            for i in range(4):
                piece = prod[:, i * 128 : (i + 1) * 128].reshape(2, 4, 8, 8, 128)
                term = piece * coef[g * 4 + i].reshape(1, 4, 1, 8, 128)
                total = term if total is None else total + term
            return total.reshape(2, 32, 8, 128)

        for g in range(4):
            total = group(g)
            for b in range(2):
                if g == 0:
                    ys[j, :, b] = total[b]
                else:
                    ys[j, :, b] += total[b]

        def send_y(i, inner):
            d = jnp.where(i < 16, (i // 4) * 8 + 4 + i % 4, ((i - 15) // 4) * 8 + (i - 15) % 4)
            tz, tmy, tcol = plane(d - 1)
            pltpu.make_async_remote_copy(
                ys.at[j, tz * 8 + tcol], yr.at[l, j, kz], y_send, y_recv,
                device_id=(tz, tmy, tcol), device_id_type=MESH,
            ).start()
            return inner

        lax.fori_loop(0, 31, send_y, 0)
        pltpu.make_async_copy(ys.at[j, z * 8 + col], yr.at[l, j, kz], y_own).start()
        return carry

    lax.fori_loop(0, 4, mode_step, 0)
    pltpu.make_async_copy(ys.at[:, 0], ys.at[:, 0], y_own).wait()
    pltpu.make_async_copy(ys.at[:, 0:31], ys.at[:, 0:31], y_recv).wait()
    pltpu.make_async_copy(sr.at[0:3], sr.at[0:3], fac_send.at[0]).wait()
    pltpu.make_async_copy(sr.at[0:3], sr.at[0:3], fac_send.at[1]).wait()
    pltpu.make_async_copy(bs.at[0:15], bs.at[0:15], b_send).wait()
    pltpu.make_async_copy(xr.at[:, :, 0:30], xr.at[:, :, 0:30], x_send).wait()
    pltpu.make_async_copy(cs.at[:, 0:7], cs.at[:, 0:7], c_send).wait()
    pltpu.make_async_copy(ys.at[:, 0:31], ys.at[:, 0:31], y_send).wait()


def finish_kernel(modes_hbm, fout_hbm, out_hbm, modes_ref, fout_ref, out_ref, in_sem, out_sem):
    load_factor = pltpu.make_async_copy(fout_hbm, fout_ref, in_sem.at[2])
    loads = [
        pltpu.make_async_copy(modes_hbm.at[:, b], modes_ref.at[b], in_sem.at[b]) for b in range(2)
    ]
    load_factor.start()
    for load in loads:
        load.start()
    load_factor.wait()
    factor = fout_ref[...].T
    blank = jnp.zeros_like(factor)
    wide = jnp.concatenate(
        [jnp.concatenate([factor, blank], axis=1), jnp.concatenate([blank, factor], axis=1)], axis=0
    )
    stores = []
    for b in range(2):
        loads[b].wait()
        modes = modes_ref.at[b].reshape(1024, 128)
        for k in range(8):
            mixed = dot(wide, modes[pl.ds(k, 128, stride=8), :], ((1,), (1,)))
            out_ref[0, b, pl.ds(k, 128, stride=8), :] = mixed[0:128]
            out_ref[1, b, pl.ds(k, 128, stride=8), :] = mixed[128:256]
        store = pltpu.make_async_copy(out_ref.at[:, b], out_hbm.at[:, b], out_sem.at[b])
        store.start()
        stores.append(store)
    for store in stores:
        store.wait()


def per_device(
    spectrum, core_tensor, input_factor, output_factor, first_factor, second_factor, third_factor
):
    spec = spectrum.reshape(2, 2, 1024, 128)
    core = jnp.transpose(core_tensor[:, :, :, 0], (0, 1, 3, 4, 2)).reshape(2, 8, 256, 64)
    anywhere = pl.BlockSpec(memory_space=pl.ANY)
    vmem = lambda *shape: pltpu.VMEM(shape, F32)
    dma = pltpu.SemaphoreType.DMA
    values = pl.pallas_call(
        kernel,
        out_shape=jax.ShapeDtypeStruct((2, 4, 16, 2, 8, 128), F32),
        in_specs=[anywhere] * 6,
        out_specs=anywhere,
        scratch_shapes=[
            vmem(2, 2, 1024, 128),
            vmem(2, 8, 256, 64),
            vmem(64, 128), vmem(64, 128), vmem(8, 16), vmem(8, 16), vmem(16, 16),
            vmem(2, 2, 4, 16, 8, 128),
            vmem(2, 4, 16, 8, 128),
            vmem(2, 4, 32, 8, 128),
            vmem(16, 2, 4, 16, 128),
            vmem(2, 4, 4, 4, 16, 128),
            vmem(2, 8, 4, 4, 16, 128),
            vmem(4, 4, 2, 2, 4, 16, 128),
            vmem(4, 32, 2, 8, 128),
            vmem(2, 8, 128),
            vmem(4, 8, 128),
            vmem(4, 8, 128),
            vmem(256, 256),
            vmem(256, 128),
            vmem(16, 32, 128),
            dma((8,)), dma((2,)), dma((2,)), dma, dma((2,)), dma((2,)), dma((2,)), dma, dma, dma, dma((4,)), dma, dma,
            dma,
        ],
        compiler_params=pltpu.CompilerParams(
            collective_id=0, has_side_effects=True, vmem_limit_bytes=63 * 1024 * 1024
        ),
    )(spec, core, input_factor.T, first_factor, second_factor, third_factor)
    out = pl.pallas_call(
        finish_kernel,
        out_shape=jax.ShapeDtypeStruct((2, 2, 1024, 128), F32),
        in_specs=[anywhere, anywhere],
        out_specs=anywhere,
        scratch_shapes=[
            vmem(2, 128, 8, 128), vmem(64, 128), vmem(2, 2, 1024, 128), dma((3,)), dma((2,)),
        ],
        compiler_params=pltpu.CompilerParams(vmem_limit_bytes=63 * 1024 * 1024),
    )(values.reshape(128, 2, 8, 128), output_factor.T)
    return out.reshape(2, 2, 128, 8, 128)


def solution(mesh):
    placed = (
        P(None, "col", None, "mx", "my"),
        P(None, "col", None, ("mx", "my"), None, None),
        P(),
        P(),
        P("mx", None),
        P("my", None),
        P(),
    )
    return jax.shard_map(
        per_device,
        mesh=mesh,
        in_specs=placed,
        out_specs=P(None, "col", None, "mx", "my"),
        check_vma=False,
    )
```

```python
import jax
import jax.numpy as jnp
from jax import lax
from jax.experimental import pallas as pl
from jax.experimental.pallas import tpu as pltpu
from jax.sharding import PartitionSpec as P

MESH = pl.DeviceIdType.MESH
F32 = jnp.float32


def exact(a, b):
    return lax.dot_general(
        a, b, (((1,), (0,)), ((), ())), precision=lax.Precision.HIGHEST, preferred_element_type=F32
    )


def split(a):
    high = a.astype(jnp.bfloat16)
    return high, (a - high.astype(F32)).astype(jnp.bfloat16)


def dot(a, b, dims=((1,), (0,))):
    (ah, al), (bh, bl) = split(a), split(b)
    one = lambda u, v: lax.dot_general(u, v, (dims, ((), ())), preferred_element_type=F32)
    return one(ah, bh) + (one(al, bh) + one(ah, bl))


def iota(shape, dim):
    return lax.broadcasted_iota(jnp.int32, shape, dim)


def kernel(
    spec_hbm, core_hbm, fin_hbm, first_hbm, second_hbm, third_hbm,
    yr,
    spec, core, fin_ref, fin, first_ref, second_ref, third_ref, xs, xp, xr, bs, br, cs, cr, ys, stage, fr, sr, m1, m2, coef,
    in_sem, fac_send, fac_recv, b_send, b_recv, p_send, p_recv, x_send, x_recv, c_send, c_recv, y_send, y_recv, y_own,
):
    z, my, col = lax.axis_index("mx"), lax.axis_index("my"), lax.axis_index("col")
    h, e = my // 2, my % 2
    l, x = col // 4, col % 4
    kz = z * 4 + x

    loads = [
        pltpu.make_async_copy(far, here, in_sem.at[n])
        for n, (far, here) in enumerate((
            (fin_hbm, fin_ref),
            (spec_hbm.at[:, 0], spec.at[:, 0]),
            (spec_hbm.at[:, 1], spec.at[:, 1]),
            (first_hbm, first_ref), (second_hbm, second_ref), (third_hbm, third_ref),
            (core_hbm.at[:, 0:4], core.at[:, 0:4]),
            (core_hbm.at[:, 4:8], core.at[:, 4:8]),
        ))
    ]
    for n in (5, 6, 0, 1, 3, 4, 7, 2):
        loads[n].start()

    rem, div = lax.rem, lax.div

    def plane(i):
        d = jnp.int32(i + 1)
        return rem(z + div(d, 8), 4), my, rem(l + rem(div(d, 4), 2), 2) * 4 + rem(x + rem(d, 4), 4)

    def square(i):
        d = jnp.int32(i + 1)
        return (
            z,
            rem(h + div(d, 4), 2) * 2 + rem(e + rem(d, 2), 2),
            rem(l + rem(div(d, 2), 2), 2) * 4 + x,
        )

    barrier = pltpu.get_barrier_semaphore()

    def hops(d):
        return (0, 1, 2, 1)[d // 8] + (d // 4) % 2 + (0, 1, 2, 1)[d % 4]

    for d in sorted([d for d in range(1, 32) if d // 4 % 2 == 0 or d == 4], key=lambda d: -hops(d)):
        pl.semaphore_signal(barrier, inc=1, device_id=plane(d - 1), device_id_type=MESH)
    for d in (4, 5, 6, 7, 3, 1):
        pl.semaphore_signal(barrier, inc=1, device_id=square(d - 1), device_id_type=MESH)

    loads[0].wait()
    for a in range(16):
        true = (a // 8) * 32 + (a % 4) * 8 + (a // 4 % 2) * 4
        fin[4 * a : 4 * a + 4, :] = fin_ref[true : true + 4, :]

    def project(b):
        loads[1 + b].wait()

        def step(n, carry):
            for k in range(4):
                k = n * 4 + k
                real = dot(fin[...], spec[0, b, pl.ds(k, 128, stride=8), :])
                imag = dot(fin[...], spec[1, b, pl.ds(k, 128, stride=8), :])
                both = jnp.concatenate([real, imag], axis=0).T
                for part in range(2):
                    rows = xs.at[part, b].reshape(512, 128)
                    rows[pl.ds(k, 64, stride=8), :] = both[part * 64 : part * 64 + 64]
            return carry

        lax.fori_loop(0, 2, step, 0)

    def swap(b):
        return pltpu.make_async_remote_copy(
            xs.at[1 - l, b], xp.at[b], p_send.at[b], p_recv.at[b],
            device_id=(z, my, (1 - l) * 4 + x), device_id_type=MESH,
        )

    for load in loads[3:5]:
        load.wait()
    stage[...] = jnp.zeros_like(stage)
    stage[0, :, 0:16] = first_ref[...]
    stage[1, :, 0:16] = second_ref[...]
    fr[pl.ds(z, 1)] = stage[0:1]
    sr[pl.ds(my, 1)] = stage[1:2]

    loads[5].wait()
    spread = jnp.where(iota((16, 256), 1) % 16 == iota((16, 256), 0), 1.0, 0.0)
    wide = exact(third_ref[...], spread)
    wide = jnp.broadcast_to(wide[:, None, :], (16, 16, 256)).reshape(256, 256)
    m1[...] = jnp.where(iota((256, 256), 0) % 16 == iota((256, 256), 1) // 16, wide, 0.0)

    def third_step(half):
        loads[6 + half].wait()
        for p in range(4):
            both = jnp.concatenate([core[0, half * 4 + p], core[1, half * 4 + p]], axis=1)
            bs[:, half, p] = dot(m1[...], both).reshape(16, 16, 128)

    def send_b(half):
        def step(i, carry):
            d = i + 1
            tz, tx = lax.rem(z + lax.div(d, 4), 4), lax.rem(x + lax.rem(d, 4), 4)
            pltpu.make_async_remote_copy(
                bs.at[tz * 4 + tx, half], br.at[half, z, x], b_send, b_recv.at[half],
                device_id=(tz, my, l * 4 + tx), device_id_type=MESH,
            ).start()
            return carry

        lax.fori_loop(0, 15, step, 0)
        br[half, z, x] = bs[kz, half]

    third_step(0)
    project(0)
    pl.semaphore_wait(barrier, 22)
    swap(0).start()
    send_b(0)
    third_step(1)
    send_b(1)
    project(1)
    swap(1).start()

    def send_first(i, carry):
        pltpu.make_async_remote_copy(
            stage.at[0], fr.at[z], fac_send.at[0], fac_recv.at[0],
            device_id=((z + i + 1) % 4, my, col), device_id_type=MESH,
        ).start()
        d = i + 1
        pltpu.make_async_remote_copy(
            stage.at[1], sr.at[my], fac_send.at[1], fac_recv.at[1],
            device_id=(z, ((h + d // 2) % 2) * 2 + (e + d % 2) % 2, col), device_id_type=MESH,
        ).start()
        return carry

    lax.fori_loop(0, 3, send_first, 0)

    pltpu.make_async_copy(sr.at[0:3], sr.at[0:3], fac_recv.at[1]).wait()
    spread2 = jnp.where(iota((128, 128), 1) % 16 == iota((128, 128), 0), 1.0, 0.0)
    wide2 = exact(sr[...].reshape(32, 128), spread2)
    wide2 = jnp.broadcast_to(wide2[:, None, :], (32, 8, 128)).reshape(256, 128)
    m2[...] = jnp.where(iota((256, 128), 0) % 8 == iota((256, 128), 1) // 16, wide2, 0.0)

    def send_x(source, sample):
        def step(i, carry):
            d = i + 1
            tz, tx = (z + d // 4) % 4, (x + d % 4) % 4
            pltpu.make_async_remote_copy(
                source.at[:, :, tz * 4 + tx], xr.at[:, :, sample], x_send, x_recv,
                device_id=(tz, my, l * 4 + tx), device_id_type=MESH,
            ).start()
            return carry

        lax.fori_loop(0, 15, step, 0)
        for b in range(2):
            for j in range(4):
                xr[b, j, sample] = source[b, j, kz]

    for half in range(2):
        pltpu.make_async_copy(bs.at[0:15, 0], bs.at[0:15, 0], b_recv.at[half]).wait()
        if half == 1:
            send_x(xs.at[l], z * 8 + col)

        def second_step(n, carry, half=half):
            for i in range(4):
                zs, pair = n * 2 + i // 2, i % 2
                block = br[half, zs, pl.ds(pair * 2, 2)].reshape(128, 128)
                part = dot(m2[...], block).reshape(8, 4, 8, 128)
                cs[half, :, :, zs, pl.ds(pair * 8, 8), :] = part
            return carry

        lax.fori_loop(0, 2, second_step, 0)

        def send_c(j, carry, half=half):
            for d in (2, 3, 4, 5, 6, 7, 1):
                tz, tmy, tcol = square(d - 1)
                pltpu.make_async_remote_copy(
                    cs.at[half, tmy * 2 + lax.div(tcol, 4), j], cr.at[j, my, l, half],
                    c_send, c_recv.at[j],
                    device_id=(tz, tmy, tcol), device_id_type=MESH,
                ).start()
            return carry

        lax.fori_loop(0, 4, send_c, 0)

        def keep_c(n, carry, half=half):
            j, zs = n // 4, n % 4
            cr[j, my, l, half, zs] = cs[half, my * 2 + l, j, zs]
            return carry

        lax.fori_loop(0, 16, keep_c, 0)

    swap(0).wait()
    swap(1).wait()
    send_x(xp, z * 8 + (1 - l) * 4 + x)

    pltpu.make_async_copy(sr.at[0:3], sr.at[0:3], fac_recv.at[0]).wait()
    for s in range(16):
        coef[s] = jnp.broadcast_to(fr[...].reshape(32, 128)[:, s : s + 1], (32, 128))
    pltpu.make_async_copy(xr.at[:, :, 0:30], xr.at[:, :, 0:30], x_recv).wait()

    sign = jnp.where(iota((64, 128), 1) < 64, -1.0, 1.0)

    def mode_step(j, carry):
        pltpu.make_async_copy(cs.at[:, 0:7, 0], cs.at[:, 0:7, 0], c_recv.at[j]).wait()
        weights = []
        for g in range(4):
            parts = []
            for i in range(4):
                top = cr[j, i, :, :, g].reshape(64, 128)
                parts.append(jnp.concatenate([top, pltpu.roll(top, 64, 1) * sign], axis=0))
            upper, lower = split(jnp.concatenate(parts, axis=1))
            weights.append((jnp.concatenate([upper, upper], axis=0), lower))
        one = lambda u, v: lax.dot_general(
            u, v, (((1,), (0,)), ((), ())), preferred_element_type=F32
        )
        for b in range(2):
            high, low = split(xr[b, j].reshape(256, 128))
            both = jnp.concatenate([high, low], axis=1)
            for g in range(4):
                prod = one(both, weights[g][0]) + one(high, weights[g][1])
                total = None
                for i in range(4):
                    piece = prod[:, i * 128 : (i + 1) * 128].reshape(4, 8, 8, 128)
                    term = piece * coef[g * 4 + i].reshape(4, 1, 8, 128)
                    total = term if total is None else total + term
                if g == 0:
                    ys[j, :, b] = total.reshape(32, 8, 128)
                else:
                    ys[j, :, b] += total.reshape(32, 8, 128)

            def send_y(i, inner, b=b):
                d = jnp.where(i < 16, (i // 4) * 8 + 4 + i % 4, ((i - 15) // 4) * 8 + (i - 15) % 4)
                tz, tmy, tcol = plane(d - 1)
                pltpu.make_async_remote_copy(
                    ys.at[j, tz * 8 + tcol, b], yr.at[l, j, kz, b], y_send, y_recv,
                    device_id=(tz, tmy, tcol), device_id_type=MESH,
                ).start()
                return inner

            lax.fori_loop(0, 31, send_y, 0)
        pltpu.make_async_copy(ys.at[j, z * 8 + col], yr.at[l, j, kz], y_own).start()
        return carry

    lax.fori_loop(0, 4, mode_step, 0)
    pltpu.make_async_copy(ys.at[:, 0], ys.at[:, 0], y_own).wait()
    pltpu.make_async_copy(ys.at[:, 0:31], ys.at[:, 0:31], y_recv).wait()
    pltpu.make_async_copy(sr.at[0:3], sr.at[0:3], fac_send.at[0]).wait()
    pltpu.make_async_copy(sr.at[0:3], sr.at[0:3], fac_send.at[1]).wait()
    pltpu.make_async_copy(bs.at[0:15], bs.at[0:15], b_send).wait()
    pltpu.make_async_copy(xr.at[:, :, 0:30], xr.at[:, :, 0:30], x_send).wait()
    pltpu.make_async_copy(cs.at[:, 0:7], cs.at[:, 0:7], c_send).wait()
    pltpu.make_async_copy(ys.at[:, 0:31], ys.at[:, 0:31], y_send).wait()


def finish_kernel(modes_hbm, fout_hbm, out_hbm, modes_ref, fout_ref, out_ref, in_sem, out_sem):
    load_factor = pltpu.make_async_copy(fout_hbm, fout_ref, in_sem.at[2])
    loads = [
        pltpu.make_async_copy(modes_hbm.at[:, b], modes_ref.at[b], in_sem.at[b]) for b in range(2)
    ]
    load_factor.start()
    for load in loads:
        load.start()
    load_factor.wait()
    factor = fout_ref[...].T
    blank = jnp.zeros_like(factor)
    wide = jnp.concatenate(
        [jnp.concatenate([factor, blank], axis=1), jnp.concatenate([blank, factor], axis=1)], axis=0
    )
    stores = []
    for b in range(2):
        loads[b].wait()
        modes = modes_ref.at[b].reshape(1024, 128)
        for k in range(8):
            mixed = dot(wide, modes[pl.ds(k, 128, stride=8), :], ((1,), (1,)))
            out_ref[0, b, pl.ds(k, 128, stride=8), :] = mixed[0:128]
            out_ref[1, b, pl.ds(k, 128, stride=8), :] = mixed[128:256]
        store = pltpu.make_async_copy(out_ref.at[:, b], out_hbm.at[:, b], out_sem.at[b])
        store.start()
        stores.append(store)
    for store in stores:
        store.wait()


def per_device(
    spectrum, core_tensor, input_factor, output_factor, first_factor, second_factor, third_factor
):
    spec = spectrum.reshape(2, 2, 1024, 128)
    core = jnp.transpose(core_tensor[:, :, :, 0], (0, 1, 3, 4, 2)).reshape(2, 8, 256, 64)
    anywhere = pl.BlockSpec(memory_space=pl.ANY)
    vmem = lambda *shape: pltpu.VMEM(shape, F32)
    dma = pltpu.SemaphoreType.DMA
    values = pl.pallas_call(
        kernel,
        out_shape=jax.ShapeDtypeStruct((2, 4, 16, 2, 8, 128), F32),
        in_specs=[anywhere] * 6,
        out_specs=anywhere,
        scratch_shapes=[
            vmem(2, 2, 1024, 128),
            vmem(2, 8, 256, 64),
            vmem(64, 128), vmem(64, 128), vmem(8, 16), vmem(8, 16), vmem(16, 16),
            vmem(2, 2, 4, 16, 8, 128),
            vmem(2, 4, 16, 8, 128),
            vmem(2, 4, 32, 8, 128),
            vmem(16, 2, 4, 16, 128),
            vmem(2, 4, 4, 4, 16, 128),
            vmem(2, 8, 4, 4, 16, 128),
            vmem(4, 4, 2, 2, 4, 16, 128),
            vmem(4, 32, 2, 8, 128),
            vmem(2, 8, 128),
            vmem(4, 8, 128),
            vmem(4, 8, 128),
            vmem(256, 256),
            vmem(256, 128),
            vmem(16, 32, 128),
            dma((8,)), dma((2,)), dma((2,)), dma, dma((2,)), dma((2,)), dma((2,)), dma, dma, dma, dma((4,)), dma, dma,
            dma,
        ],
        compiler_params=pltpu.CompilerParams(
            collective_id=0, has_side_effects=True, vmem_limit_bytes=63 * 1024 * 1024
        ),
    )(spec, core, input_factor.T, first_factor, second_factor, third_factor)
    out = pl.pallas_call(
        finish_kernel,
        out_shape=jax.ShapeDtypeStruct((2, 2, 1024, 128), F32),
        in_specs=[anywhere, anywhere],
        out_specs=anywhere,
        scratch_shapes=[
            vmem(2, 128, 8, 128), vmem(64, 128), vmem(2, 2, 1024, 128), dma((3,)), dma((2,)),
        ],
        compiler_params=pltpu.CompilerParams(vmem_limit_bytes=63 * 1024 * 1024),
    )(values.reshape(128, 2, 8, 128), output_factor.T)
    return out.reshape(2, 2, 128, 8, 128)


def solution(mesh):
    placed = (
        P(None, "col", None, "mx", "my"),
        P(None, "col", None, ("mx", "my"), None, None),
        P(),
        P(),
        P("mx", None),
        P("my", None),
        P(),
    )
    return jax.shard_map(
        per_device,
        mesh=mesh,
        in_specs=placed,
        out_specs=P(None, "col", None, "mx", "my"),
        check_vma=False,
    )
```
